128 devices in a mesh: date: 4 (over x), pix: 32 (over y, z, core).
Axes of the slice: x: 4, y: 4, z: 4, core: 2. Of those that a mesh axis runs over, the one named last changes fastest.
Arguments:
- stack: bfloat16 [64, 7, 256, 4096], P('date', None, None, 'pix'), may hold values from -8 to 8
- quality: int32 [64, 256, 4096], P('date', None, 'pix'), may hold values from 0 to 1073741823
- days: int32 [64], P('date'), may hold values from 8 to 1536, as said below
Outputs:
- coef: float32 [7, 8, 256, 4096], P(None, None, 'pix', 'date')
- score: float32 [7, 256, 4096], P(None, 'pix', 'date')
The draws below stay inside these ranges and needn't reach their ends.
Inputs may be any that keep to these rules, and one draw needn't show every extreme that they name: `days`: strictly increasing.
All inputs are finite; a program needn't handle non-finite values.
Results may differ from the reference program's by a relative error of at most 0.0003.
Values may be sent and summed in bfloat16 or wider, within the bound.
A program may use at most 256 MiB of HBM per device.

```python
import jax
import jax.numpy as jnp
from jax import lax

DATES = 64
BANDS = 7
HARM = 8
ROWS = 256
COLS = 4096


def make_days(key):
    inner_count = 24 * DATES - 9
    order = jax.random.permutation(jax.random.fold_in(key, 11), inner_count)
    chosen = jnp.sort(order[:DATES - 2]).astype(jnp.int32) + 9
    first = jnp.full((1,), 8, dtype=jnp.int32)
    last = jnp.full((1,), 24 * DATES, dtype=jnp.int32)
    return jnp.concatenate([first, chosen, last]).astype(jnp.int32)


def design_matrix_drawn(days):
    moment_t = days.astype(jnp.float32)
    columns = [jnp.ones_like(moment_t), (moment_t - 512.0) / 512.0]
    for order in range(1, 4):
        phase = 2.0 * jnp.pi * order * moment_t / 365.25
        columns.append(jnp.cos(phase))
        columns.append(jnp.sin(phase))
    return jnp.stack(columns, 1)


def draw_days(key, part):
    return make_days(key)


def draw_quality(key, part):
    shape = (DATES, ROWS, COLS)
    bits = jax.random.randint(jax.random.fold_in(key, 21), shape, 0, 2 ** 30)
    rows = jnp.arange(ROWS, dtype=jnp.int32)
    cols = jnp.arange(COLS, dtype=jnp.int32)
    row_limit = 300 * rows // max(ROWS - 1, 1)
    col_limit = 300 * cols // max(COLS - 1, 1)
    limit = 200 + row_limit[:, None] + col_limit[None, :]
    rolled = jax.random.randint(jax.random.fold_in(key, 22), shape, 0, 1000)
    cloud = (rolled < limit[None, :, :]).astype(jnp.int32)
    return (bits - jnp.bitwise_and(bits, 8) + 8 * cloud).astype(jnp.int32)


def draw_stack(key, part):
    design = design_matrix_drawn(make_days(key))
    coefs = 0.6 * jax.random.normal(jax.random.fold_in(key, 31), (HARM, BANDS, ROWS, COLS), jnp.float32)
    rough = jax.random.uniform(jax.random.fold_in(key, 32), (BANDS, ROWS, COLS), jnp.float32, 0.5, 1.5)
    rows = jnp.arange(ROWS, dtype=jnp.float32)
    cols = jnp.arange(COLS, dtype=jnp.float32)
    row_scale = 0.15 * jnp.power(3.2, rows / max(ROWS - 1, 1))
    col_scale = jnp.power(3.2, cols / max(COLS - 1, 1))
    scale_map = row_scale[:, None] * col_scale[None, :]
    shape = (DATES, BANDS, ROWS, COLS)
    noise = jax.random.normal(jax.random.fold_in(key, 33), shape, jnp.float32)
    signal = jnp.einsum('tk,kbrc->tbrc', design, coefs)
    values = signal + noise * rough[None] * scale_map[None, None, :, :]
    return jnp.clip(values, -8.0, 8.0).astype(jnp.bfloat16)


def setup_inputs(seed: int = 0) -> dict:
    key_of = jax.random.split(jax.random.key(seed), 4)
    stack = draw_stack(jax.random.fold_in(key_of[3], 71), 0)
    quality = draw_quality(jax.random.fold_in(key_of[3], 71), 0)
    days = draw_days(jax.random.fold_in(key_of[3], 71), 0)
    return {"stack": stack, "quality": quality, "days": days}


RIDGE_TERM = 1.0
PAIR_LIST = [(first, second) for first in range(8) for second in range(first, 8)]

def design_matrix(days):
    moment_t = days.astype(jnp.float32)
    columns = [jnp.ones_like(moment_t), (moment_t - 512.0) / 512.0]
    for order in range(1, 4):
        phase = 2.0 * jnp.pi * order * moment_t / 365.25
        columns.append(jnp.cos(phase))
        columns.append(jnp.sin(phase))
    return jnp.stack(columns, 1)

def weights(quality):
    cloud = jnp.bitwise_and(jnp.right_shift(quality, 3), 1)
    level = jnp.bitwise_and(jnp.right_shift(quality, 8), 3)
    return (1 - cloud).astype(jnp.float32) / (1.0 + level.astype(jnp.float32))

def reference(stack, quality, days):
    design = design_matrix(days)
    products = jnp.stack([design[:, first] * design[:, second] for first, second in PAIR_LIST], 1)
    index_table = [[0] * 8 for first in range(8)]
    for number, pair in enumerate(PAIR_LIST):
        index_table[pair[0]][pair[1]] = number
        index_table[pair[1]][pair[0]] = number
    index_array = jnp.array(index_table, dtype=jnp.int32)
    high = lax.Precision.HIGHEST

    def row_fit(row):
        values = lax.dynamic_slice_in_dim(stack, row, 1, 2)[:, :, 0, :].astype(jnp.float32)
        bits = lax.dynamic_slice_in_dim(quality, row, 1, 1)[:, 0, :]
        weight = weights(bits)
        gram = jnp.dot(products.T, weight, precision=high)
        moment = jnp.einsum('tk,tbc->kbc', design, weight[:, None, :] * values, precision=high)
        full = jnp.transpose(gram[index_array], (2, 0, 1)) + RIDGE_TERM * jnp.eye(8, dtype=jnp.float32)
        solved = jnp.linalg.solve(full, jnp.transpose(moment, (2, 0, 1)))
        coef_row = jnp.transpose(solved, (1, 2, 0))
        fitted = jnp.einsum('tk,kbc->tbc', design, coef_row, precision=high)
        ssr = lax.optimization_barrier(jnp.sum(weight[:, None, :] * (values - fitted) ** 2, 0))
        return (coef_row, ssr, lax.optimization_barrier(jnp.sum(weight, 0)))
    coef_rows, ssr, wsum = lax.map(row_fit, jnp.arange(ROWS, dtype=jnp.int32))
    sigma2 = lax.optimization_barrier(jnp.sum(ssr, (0, 2))) / jnp.sum(wsum)
    score = jnp.sqrt(ssr / (wsum[:, None, :] + 1.0)) / jnp.sqrt(sigma2)[None, :, None]
    return (jnp.transpose(coef_rows, (2, 1, 0, 3)), jnp.transpose(score, (1, 0, 2)))
```

```python
import jax
import jax.numpy as jnp
from jax import lax
from jax.experimental import pallas as pl
from jax.experimental.pallas import tpu as pltpu
from jax.sharding import PartitionSpec as P

MESH = pl.DeviceIdType.MESH
F32 = jnp.float32
BF16 = jnp.bfloat16

BANDS = 7
GROUP = 16
PARTS = 4
DPART = GROUP // PARTS
CHUNKS = 4
STEPS = CHUNKS * PARTS
SCALE = 12.0
PAIRS = [(i, j) for i in range(8) for j in range(i, 8)]


def pair(i, j):
    return PAIRS.index((min(i, j), max(i, j)))


def design_matrix(days):
    moment_t = days.astype(F32)
    columns = [jnp.ones_like(moment_t), (moment_t - 512.0) / 512.0]
    for order in range(1, 4):
        phase = 2.0 * jnp.pi * order * moment_t / 365.25
        columns.append(jnp.cos(phase))
        columns.append(jnp.sin(phase))
    return jnp.stack(columns, 1)


def fit_kernel(
    stack, quality, design, coef_out, score_out,
    mid, midw, far, farw, wout, qv, dbuf, dfull, acc, gram, low, res, sres, sstage, arsum, arsrc, arbuf,
    q_sem, l_sem, d_loc, ys, yr, yws, ywr, xs, xr, xws, xwr, ds_, dr_, cs, cr, ss, sr, c_loc, as_, ar_,
):
    x = lax.axis_index("date")
    p = lax.axis_index("pix")
    y = lax.div(p, 8)
    z = lax.rem(lax.div(p, 2), 4)
    c = lax.rem(p, 2)

    def pix(py, pz, pc):
        return (py * 4 + pz) * 2 + pc

    y_peers = [(x, pix(lax.rem(y + t, 4), z, c)) for t in range(1, 4)]
    x_peers = [(lax.rem(x + t, 4), p) for t in range(1, 4)]
    z_peers = [
        (x, pix(y, lax.rem(z + e // 2, 4), lax.rem(c + e % 2, 2))) for e in range(1, 8)
    ]

    def remote(src, dst, send, recv, dev):
        return pltpu.make_async_remote_copy(
            src_ref=src, dst_ref=dst, send_sem=send, recv_sem=recv,
            device_id=dev, device_id_type=MESH,
        )

    q_copy = pltpu.make_async_copy(quality, qv, q_sem)
    q_copy.start()
    d_copy = pltpu.make_async_copy(design, dbuf.at[0], d_loc)
    d_copy.start()

    barrier = pltpu.get_barrier_semaphore()
    for dev in y_peers + x_peers + z_peers:
        pl.semaphore_signal(barrier, inc=1, device_id=dev, device_id_type=MESH)
    pl.semaphore_wait(barrier, 13)

    def chunk_row(ry, t):
        return pl.multiple_of(ry * 64 + lax.rem(z + 1 + t, 4) * 16, 16)

    def y_copy(s, t, q, tp):
        ry = lax.rem(y + tp, 4)
        return remote(
            stack.at[pl.ds(q * DPART, DPART), :, pl.ds(chunk_row(ry, t), 16), :],
            mid.at[4 - tp, t, pl.ds(q * DPART, DPART)],
            ys.at[s, tp - 1], yr.at[s, 3 - tp], y_peers[tp - 1],
        )

    def y_local(s, t, q):
        return pltpu.make_async_copy(
            stack.at[pl.ds(q * DPART, DPART), :, pl.ds(chunk_row(y, t), 16), :],
            mid.at[0, t, pl.ds(q * DPART, DPART)],
            l_sem.at[s],
        )

    def yw_copy(t, tp):
        return remote(
            wout.at[tp - 1, t], midw.at[4 - tp, t],
            yws.at[t, tp - 1], ywr.at[t, 3 - tp], y_peers[tp - 1],
        )

    def x_copy(s, t, q, tp):
        i = lax.rem(x + tp - y + 4, 4)
        return remote(
            mid.at[i, t, pl.ds(q * DPART, DPART)],
            far.at[3 - tp, t, pl.ds(q * DPART, DPART)],
            xs.at[s, tp - 1], xr.at[s, 3 - tp], x_peers[tp - 1],
        )

    def xw_copy(t, tp):
        i = lax.rem(x + tp - y + 4, 4)
        return remote(
            midw.at[i, t], farw.at[3 - tp, t],
            xws.at[t, tp - 1], xwr.at[t, 3 - tp], x_peers[tp - 1],
        )

    def d_remote(tp):
        return remote(design, dbuf.at[4 - tp], ds_.at[tp - 1], dr_.at[3 - tp], x_peers[tp - 1])

    def y_start(s):
        t = lax.div(s, PARTS)
        q = lax.rem(s, PARTS)
        for tp in (2, 1, 3):
            y_copy(s, t, q, tp).start()
        y_local(s, t, q).start()

    y_start(0)
    for tp in range(1, 4):
        d_remote(tp).start()

    q_copy.wait()

    def encode(n, carry):
        tp = lax.div(n, CHUNKS)
        t = lax.rem(n, CHUNKS)
        bits = qv[:, pl.ds(chunk_row(lax.rem(y + tp, 4), t), 16), :]
        level = jnp.bitwise_and(jnp.right_shift(bits, 8), 3)
        clear = jnp.bitwise_and(bits, 8) == 0
        code = jnp.where(level == 0, 12.0, jnp.where(level == 1, 6.0, jnp.where(level == 2, 4.0, 3.0)))
        code = jnp.where(clear, code, 0.0).astype(BF16)

        @pl.when(tp == 0)
        def _():
            midw[0, t] = code

        @pl.when(tp > 0)
        def _():
            wout[tp - 1, t] = code

        return carry

    lax.fori_loop(0, 4 * CHUNKS, encode, 0)

    def yw_start(t):
        for tp in (2, 1, 3):
            yw_copy(t, tp).start()

    yw_start(0)
    y_start(1)
    y_start(2)

    d_copy.wait()
    for tp in range(1, 4):
        d_remote(tp).wait_recv()

    def spread(n, carry):
        g = lax.div(n, GROUP)
        d = lax.rem(n, GROUP)
        for i in range(8):
            dfull[g, d, i] = jnp.broadcast_to(dbuf[g, d, pl.ds(i, 1), :], (8, 128))
        return carry

    lax.fori_loop(0, 4 * GROUP, spread, 0)
    arsum[...] = jnp.zeros_like(arsum)

    home = lax.rem(x - y + 4, 4)

    def column(g, d, i):
        v = dfull[g, d, i]
        return jnp.concatenate([v, v], 0)

    def groups(t):
        out = [(mid.at[home, t], midw.at[home, t])]
        for j in range(1, 4):
            out.append((far.at[j - 1, t], farw.at[j - 1, t]))
        return out

    def factor(t):
        refs = groups(t)
        for rows in ((0, 1), (2, 3), (4, 5, 6, 7)):
            wanted = [(i, j) for i in rows for j in range(i, 8)]

            def add(d, sums, rows=rows, wanted=wanted):
                sums = list(sums)
                for g in range(4):
                    w = refs[g][1][d].astype(F32)
                    cols = {k: column(g, d, k) for k in range(rows[0], 8)}
                    for i in rows:
                        wd = w if i == 0 else w * cols[i]
                        for j in range(i, 8):
                            n = wanted.index((i, j))
                            sums[n] = sums[n] + (wd if j == 0 else wd * cols[j])
                return tuple(sums)

            sums = lax.fori_loop(
                0, GROUP, add, tuple(jnp.zeros((16, 128), F32) for _ in wanted)
            )
            for n, (i, j) in enumerate(wanted):
                gram[pair(i, j)] = sums[n]
        for half in (0, 8):
            lower = {}
            for j in range(8):
                total = gram[pair(j, j), half:half + 8, :] + SCALE
                for k in range(j):
                    total = total - lower[j, k] * lower[j, k]
                inverse = 1.0 / jnp.sqrt(total)
                low[pair(j, j), half:half + 8, :] = inverse
                for i in range(j + 1, 8):
                    total = gram[pair(j, i), half:half + 8, :]
                    for k in range(j):
                        total = total - lower[i, k] * lower[j, k]
                    lower[i, j] = total * inverse
                    low[pair(j, i), half:half + 8, :] = lower[i, j]
        arsum[7] = arsum[7] + gram[0, 0:8, :] + gram[0, 8:16, :]

    def moments(t, q):
        refs = groups(t)

        def band(b, carry):
            sums = [acc[b, n] for n in range(9)]
            for g in range(4):
                for dd in range(DPART):
                    d = q * DPART + dd
                    v = refs[g][0][d, b].astype(F32)
                    wv = refs[g][1][d].astype(F32) * v
                    sums[8] = sums[8] + wv * v
                    sums[0] = sums[0] + wv
                    for i in range(1, 8):
                        sums[i] = sums[i] + wv * column(g, d, i)
            for n in range(9):
                acc[b, n] = sums[n]
            return carry

        lax.fori_loop(0, BANDS, band, 0)

    def solve(t):
        def band(b, carry):
            fit = []
            explained = None
            for i in range(8):
                total = acc[b, i]
                for k in range(i):
                    total = total - low[pair(k, i)] * fit[k]
                total = total * low[pair(i, i)]
                fit.append(total)
                explained = total * total if i == 0 else explained + total * total
            for i in range(7, -1, -1):
                total = fit[i]
                for k in range(i + 1, 8):
                    total = total - low[pair(i, k)] * fit[k]
                total = total * low[pair(i, i)]
                fit[i] = total
                res[t, 0, b, i] = total[0:8, :]
                res[t, 1, b, i] = total[8:16, :]
                explained = explained + SCALE * total * total
            ssr = jnp.maximum(acc[b, 8] - explained, 0.0)
            arsum[b] = arsum[b] + ssr[0:8, :] + ssr[8:16, :]
            ratio = jnp.sqrt(ssr / (gram[0] + SCALE))
            sres[t, 0, b] = ratio[0:8, :]
            sres[t, 1, b] = ratio[8:16, :]
            return carry

        lax.fori_loop(0, BANDS, band, 0)

    def lanes(pz, pc):
        return pl.ds(pl.multiple_of((pz * 2 + pc) * 128, 128), 128)

    def out_copies(t, half, slot, dev):
        return (
            remote(sres.at[t, half], sstage.at[z * 2 + c], ss.at[t, half], sr.at[t, slot], dev),
            remote(res.at[t, half], coef_out.at[:, :, :, lanes(z, c)], cs.at[t, half], cr.at[t, slot], dev),
        )

    def step(s, carry):
        @pl.when(s < STEPS)
        def _():
            t = lax.div(s, PARTS)
            q = lax.rem(s, PARTS)

            @pl.when(q == 0)
            def _():
                for tp in range(1, 4):
                    yw_copy(t, tp).wait_recv()
                for tp in (2, 1, 3):
                    xw_copy(t, tp).start()

            y_local(s, t, q).wait()
            for tp in range(1, 4):
                y_copy(s, t, q, tp).wait_recv()
            for tp in (2, 1, 3):
                x_copy(s, t, q, tp).start()

            @pl.when(s + 3 < STEPS)
            def _():
                @pl.when(lax.rem(s + 3, PARTS) == 0)
                def _():
                    yw_start(lax.div(s + 3, PARTS))

                y_start(s + 3)

        @pl.when(s > 0)
        def _():
            n = s - 1
            t = lax.div(n, PARTS)
            q = lax.rem(n, PARTS)

            @pl.when(q == 0)
            def _():
                for tp in range(1, 4):
                    xw_copy(t, tp).wait_recv()
                acc[...] = jnp.zeros_like(acc)
                factor(t)

            for tp in range(1, 4):
                x_copy(n, t, q, tp).wait_recv()
            moments(t, q)

            @pl.when(q == PARTS - 1)
            def _():
                solve(t)

                @pl.when(t < CHUNKS - 1)
                def _():
                    for half in range(2):
                        dev = (x, pix(y, lax.rem(z + 1 + t, 4), half))
                        for copy in out_copies(t, half, c, dev):
                            copy.start()

        return carry

    lax.fori_loop(0, STEPS + 1, step, 0)

    last = CHUNKS - 1
    twin = (x, pix(y, z, 1 - c))
    arsrc[0] = jnp.sum(arsum[...], axis=1)

    def gather(stage, peers, first):
        copies = [
            remote(arsrc.at[stage], arbuf.at[first + n], as_.at[first + n], ar_.at[first + n], dev)
            for n, dev in enumerate(peers)
        ]
        for copy in copies:
            copy.start()
        return copies

    copies = gather(0, z_peers, 0)
    twin_copies = out_copies(last, 1 - c, 0, twin)
    for copy in twin_copies:
        copy.start()
    own = pltpu.make_async_copy(res.at[last, c], coef_out.at[:, :, :, lanes(z, c)], c_loc)
    own.start()
    sstage[z * 2 + c] = sres[last, c]
    started = list(copies)
    for stage, peers, first in ((1, y_peers, 7), (2, x_peers, 10)):
        for copy in copies:
            copy.wait_recv()
        total = arsrc[stage - 1]
        for n in range(len(copies)):
            total = total + arbuf[first - len(copies) + n]
        arsrc[stage] = total
        copies = gather(stage, peers, first)
        started += copies
    for copy in copies:
        copy.wait_recv()
    total = arsrc[2]
    for n in range(3):
        total = total + arbuf[10 + n]
    total = jnp.sum(total, axis=1, keepdims=True)
    inverse = 1.0 / jnp.sqrt(total / total[7:8, :])

    for t in range(CHUNKS - 1):
        for half in range(2):
            dev = (x, pix(y, lax.rem(z + 1 + t, 4), half))
            for copy in out_copies(t, half, half, dev):
                copy.wait()
    for copy in twin_copies:
        copy.wait()
    own.wait()
    for b in range(BANDS):
        factor_b = jnp.broadcast_to(inverse[b:b + 1, :], (8, 128))
        for n in range(8):
            score_out[b, :, n * 128:(n + 1) * 128] = sstage[n, b] * factor_b

    for copy in started:
        copy.wait_send()
    for tp in range(1, 4):
        d_remote(tp).wait_send()

    def drain(s, carry):
        t = lax.div(s, PARTS)
        q = lax.rem(s, PARTS)
        for tp in range(1, 4):
            y_copy(s, t, q, tp).wait_send()
            x_copy(s, t, q, tp).wait_send()

        @pl.when(q == 0)
        def _():
            for tp in range(1, 4):
                yw_copy(t, tp).wait_send()
                xw_copy(t, tp).wait_send()

        return carry

    lax.fori_loop(0, STEPS, drain, 0)


def local(stack, quality, days):
    design = jnp.broadcast_to(design_matrix(days)[:, :, None], (GROUP, 8, 128))
    dma = pltpu.SemaphoreType.DMA
    vmem = pltpu.VMEM
    hbm = pl.BlockSpec(memory_space=pltpu.HBM)
    return pl.pallas_call(
        fit_kernel,
        out_shape=(
            jax.ShapeDtypeStruct((BANDS, 8, 8, 1024), F32),
            jax.ShapeDtypeStruct((BANDS, 8, 1024), F32),
        ),
        in_specs=[hbm, hbm, hbm],
        out_specs=(hbm, pl.BlockSpec(memory_space=pltpu.VMEM)),
        scratch_shapes=[
            vmem((4, CHUNKS, GROUP, BANDS, 16, 128), BF16),
            vmem((4, CHUNKS, GROUP, 16, 128), BF16),
            vmem((3, CHUNKS, GROUP, BANDS, 16, 128), BF16),
            vmem((3, CHUNKS, GROUP, 16, 128), BF16),
            vmem((3, CHUNKS, GROUP, 16, 128), BF16),
            vmem((GROUP, 256, 128), jnp.int32),
            vmem((4, GROUP, 8, 128), F32),
            vmem((4, GROUP, 8, 8, 128), F32),
            vmem((BANDS, 9, 16, 128), F32),
            vmem((36, 16, 128), F32),
            vmem((36, 16, 128), F32),
            vmem((CHUNKS, 2, BANDS, 8, 8, 128), F32),
            vmem((CHUNKS, 2, BANDS, 8, 128), F32),
            vmem((8, BANDS, 8, 128), F32),
            vmem((8, 8, 128), F32),
            vmem((3, 8, 128), F32),
            vmem((13, 8, 128), F32),
            dma, dma((STEPS,)), dma,
            dma((STEPS, 3)), dma((STEPS, 3)), dma((CHUNKS, 3)), dma((CHUNKS, 3)),
            dma((STEPS, 3)), dma((STEPS, 3)), dma((CHUNKS, 3)), dma((CHUNKS, 3)),
            dma((3,)), dma((3,)),
            dma((CHUNKS, 2)), dma((CHUNKS, 2)), dma((CHUNKS, 2)), dma((CHUNKS, 2)),
            dma, dma((13,)), dma((13,)),
        ],
        compiler_params=pltpu.CompilerParams(
            collective_id=0, has_side_effects=True, vmem_limit_bytes=48 * 1024 * 1024
        ),
        name="fit",
    )(stack, quality, design)


def solution(mesh):
    return jax.shard_map(
        local,
        mesh=mesh,
        in_specs=(P("date", None, None, "pix"), P("date", None, "pix"), P("date")),
        out_specs=(P(None, None, "pix", "date"), P(None, "pix", "date")),
        check_vma=False,
    )
```

```python
import jax
import jax.numpy as jnp
from jax import lax
from jax.experimental import pallas as pl
from jax.experimental.pallas import tpu as pltpu
from jax.sharding import PartitionSpec as P

MESH = pl.DeviceIdType.MESH
F32 = jnp.float32
BF16 = jnp.bfloat16

BANDS = 7
GROUP = 16
PARTS = 4
DPART = GROUP // PARTS
CHUNKS = 4
STEPS = CHUNKS * PARTS
AHEAD = 3
LAG = 3
SCALE = 12.0
PAIRS = [(i, j) for i in range(8) for j in range(i, 8)]


def pair(i, j):
    return PAIRS.index((min(i, j), max(i, j)))


def design_matrix(days):
    moment_t = days.astype(F32)
    columns = [jnp.ones_like(moment_t), (moment_t - 512.0) / 512.0]
    for order in range(1, 4):
        phase = 2.0 * jnp.pi * order * moment_t / 365.25
        columns.append(jnp.cos(phase))
        columns.append(jnp.sin(phase))
    return jnp.stack(columns, 1)


def fit_kernel(
    stack, quality, design, coef_out, score_out,
    mid, midw, far, farw, carry, carryw, wout, qv, dbuf, dfull, own_sums, pass_sums, got_sums,
    gram, low, res, sres, yres, ysres, sstage, arsum, arsrc, arbuf,
    q_sem, l_sem, d_loc, ys, yr, yws, ywr, a_s, a_r, b_s, b_r, xs, xr, wa_s, wa_r, ws, wr, sm_s, sm_r,
    ds_, dr_, e_s, e_r, fc, fs, cs, cr, ss, sr, c_loc, as_, ar_,
):
    x = lax.axis_index("date")
    p = lax.axis_index("pix")
    y = lax.div(p, 8)
    z = lax.rem(lax.div(p, 2), 4)
    c = lax.rem(p, 2)
    last = CHUNKS - 1

    def pix(py, pz, pc):
        return (py * 4 + pz) * 2 + pc

    def right(n):
        return (lax.rem(x + n, 4), p)

    fore = 1 + 2 * c
    back = 3 - 2 * c
    fore_dev = right(fore)
    back_dev = right(back)
    home = lax.rem(x - y + 4, 4)
    fore_slot = lax.rem(x + fore - y + 4, 4)
    back_slot = lax.rem(x + back - y + 4, 4)
    far_slot = lax.rem(x + 2 - y + 4, 4)
    turn = lax.rem(x + 2 * c, 4)

    y_peers = [(x, pix(lax.rem(y + t, 4), z, c)) for t in range(1, 4)]
    x_peers = [right(t) for t in range(1, 4)]
    plane_peers = [
        (lax.rem(x + n // 4, 4), pix(lax.rem(y + n % 4, 4), z, c)) for n in range(1, 16)
    ]
    z_peers = [
        (x, pix(y, lax.rem(z + e // 2, 4), lax.rem(c + e % 2, 2))) for e in range(1, 8)
    ]

    def remote(src, dst, send, recv, dev):
        return pltpu.make_async_remote_copy(
            src_ref=src, dst_ref=dst, send_sem=send, recv_sem=recv,
            device_id=dev, device_id_type=MESH,
        )

    def dates(q):
        return pl.ds(q * DPART, DPART)

    def chunk_row(ry, t):
        return pl.multiple_of(ry * 64 + lax.rem(z + 1 + t, 4) * 16, 16)

    def first_local(q, i):
        ry = lax.rem(y + i + 2 * c, 4)
        return pltpu.make_async_copy(
            stack.at[dates(q), :, pl.ds(chunk_row(ry, 0), 16), :],
            mid.at[i, 0, dates(q)],
            l_sem.at[q, i],
        )

    def y_local(s, t, q):
        return pltpu.make_async_copy(
            stack.at[dates(q), :, pl.ds(chunk_row(y, t), 16), :],
            mid.at[0, t, dates(q)],
            l_sem.at[s, 0],
        )

    def y_copy(s, t, q, tp):
        ry = lax.rem(y + tp, 4)
        return remote(
            stack.at[dates(q), :, pl.ds(chunk_row(ry, t), 16), :],
            mid.at[4 - tp, t, dates(q)],
            ys.at[s, tp - 1], yr.at[s, 3 - tp], y_peers[tp - 1],
        )

    def yw_copy(t, tp):
        return remote(
            wout.at[tp - 1, t], midw.at[4 - tp, t],
            yws.at[t, tp - 1], ywr.at[t, 3 - tp], y_peers[tp - 1],
        )

    def a_copy(s, t, q):
        return remote(mid.at[far_slot, t, dates(q)], carry.at[t, dates(q)], a_s.at[s], a_r.at[s], fore_dev)

    def b_copy(s, t, q):
        return remote(mid.at[back_slot, t, dates(q)], far.at[2 * c, t, dates(q)], b_s.at[s], b_r.at[s], back_dev)

    def x_copy(q, tp):
        i = lax.rem(x + tp - y + 4, 4)
        return remote(
            mid.at[i, last, dates(q)], far.at[3 - tp, last, dates(q)],
            xs.at[q, tp - 1], xr.at[q, 3 - tp], x_peers[tp - 1],
        )

    def xw_copy(tp):
        i = lax.rem(x + tp - y + 4, 4)
        return remote(
            midw.at[i, last], farw.at[3 - tp, last],
            ws.at[last, tp - 1], wr.at[last, 3 - tp], x_peers[tp - 1],
        )

    def wa_copy(t):
        return remote(midw.at[far_slot, t], carryw.at[t], wa_s.at[t], wa_r.at[t], fore_dev)

    def wb_copy(t):
        return remote(midw.at[back_slot, t], farw.at[2 * c, t], ws.at[t, 0], wr.at[t, 2 * c], back_dev)

    def wc_copy(t):
        return remote(midw.at[fore_slot, t], farw.at[2 - 2 * c, t], ws.at[t, 1], wr.at[t, 2 - 2 * c], fore_dev)

    def wd_copy(t):
        return remote(carryw.at[t], farw.at[1, t], ws.at[t, 2], wr.at[t, 1], fore_dev)

    def sum_copy(t):
        return remote(pass_sums.at[t], got_sums.at[t], sm_s.at[t], sm_r.at[t], fore_dev)

    def d_remote(tp):
        return remote(design, dbuf.at[4 - tp], ds_.at[tp - 1], dr_.at[3 - tp], x_peers[tp - 1])

    def y_start(s):
        t = lax.div(s, PARTS)
        q = lax.rem(s, PARTS)
        for tp in (2, 1, 3):
            y_copy(s, t, q, tp).start()
        y_local(s, t, q).start()

    def yw_start(t):
        for tp in (2, 1, 3):
            yw_copy(t, tp).start()

    for i in range(4):
        first_local(0, i).start()
    q_copy = pltpu.make_async_copy(quality, qv, q_sem)
    q_copy.start()
    for q in range(1, PARTS):
        for i in range(4):
            first_local(q, i).start()
    d_copy = pltpu.make_async_copy(design, dbuf.at[0], d_loc)
    d_copy.start()

    barrier = pltpu.get_barrier_semaphore()
    for dev in y_peers + x_peers + z_peers:
        pl.semaphore_signal(barrier, inc=1, device_id=dev, device_id_type=MESH)
    pl.semaphore_wait(barrier, 13)

    y_start(PARTS)
    for i in range(4):
        first_local(0, i).wait()
    a_copy(0, 0, 0).start()
    b_copy(0, 0, 0).start()
    for tp in range(1, 4):
        d_remote(tp).start()

    q_copy.wait()

    def encode(n, carried):
        t = lax.div(n, 4)
        tp = lax.rem(n, 4)
        ry = lax.rem(y + tp + jnp.where(t == 0, 2 * c, 0), 4)
        bits = qv[:, pl.ds(chunk_row(ry, t), 16), :]
        level = jnp.bitwise_and(jnp.right_shift(bits, 8), 3)
        clear = jnp.bitwise_and(bits, 8) == 0
        code = jnp.where(level == 0, 12.0, jnp.where(level == 1, 6.0, jnp.where(level == 2, 4.0, 3.0)))
        code = jnp.where(clear, code, 0.0).astype(BF16)
        kept = jnp.logical_or(t == 0, tp == 0)

        @pl.when(kept)
        def _():
            midw[tp, t] = code

        @pl.when(jnp.logical_not(kept))
        def _():
            wout[tp - 1, t] = code

        return carried

    lax.fori_loop(0, 4 * CHUNKS, encode, 0)
    yw_start(1)
    for s in range(1, AHEAD):
        y_start(PARTS + s)
    arsum[...] = jnp.zeros_like(arsum)

    def column(g, d, i):
        v = dfull[g, d, i]
        return jnp.concatenate([v, v], 0)

    def columns():
        d_copy.wait()
        for tp in range(1, 4):
            d_remote(tp).wait_recv()

        def spread(n, carried):
            g = lax.div(n, GROUP)
            d = lax.rem(n, GROUP)
            row = dbuf[g, pl.ds(d, 1), :]
            for i in range(8):
                dfull[g, d, i] = jnp.broadcast_to(row[:, i:i + 1], (8, 128))
            return carried

        lax.fori_loop(0, 4 * GROUP, spread, 0)

    def factor(t):
        codes = [midw.at[home, t]] + [farw.at[j, t] for j in range(3)]
        for rows in ((0, 1), (2, 3), (4, 5, 6, 7)):
            wanted = [(i, j) for i in rows for j in range(i, 8)]

            def add(d, sums, rows=rows, wanted=wanted):
                sums = list(sums)
                for g in range(4):
                    w = codes[g][d].astype(F32)
                    cols = {k: column(g, d, k) for k in range(rows[0], 8)}
                    for i in rows:
                        wd = w if i == 0 else w * cols[i]
                        for j in range(i, 8):
                            n = wanted.index((i, j))
                            sums[n] = sums[n] + (wd if j == 0 else wd * cols[j])
                return tuple(sums)

            sums = lax.fori_loop(
                0, GROUP, add, tuple(jnp.zeros((16, 128), F32) for _ in wanted)
            )
            for n, (i, j) in enumerate(wanted):
                gram[t, pair(i, j)] = sums[n]
        for half in (0, 8):
            lower = {}
            for j in range(8):
                total = gram[t, pair(j, j), half:half + 8, :] + SCALE
                for k in range(j):
                    total = total - lower[j, k] * lower[j, k]
                inverse = 1.0 / jnp.sqrt(total)
                low[t, pair(j, j), half:half + 8, :] = inverse
                for i in range(j + 1, 8):
                    total = gram[t, pair(j, i), half:half + 8, :]
                    for k in range(j):
                        total = total - lower[i, k] * lower[j, k]
                    lower[i, j] = total * inverse
                    low[t, pair(j, i), half:half + 8, :] = lower[i, j]
        arsum[7] = arsum[7] + gram[t, 0, 0:8, :] + gram[t, 0, 8:16, :]

    def moments(acc, refs, q):
        def band(b, carried):
            sums = [acc[b, n] for n in range(9)]
            for values, codes, g in refs:
                for dd in range(DPART):
                    d = q * DPART + dd
                    v = values[d, b].astype(F32)
                    wv = codes[d].astype(F32) * v
                    sums[8] = sums[8] + wv * v
                    sums[0] = sums[0] + wv
                    for i in range(1, 8):
                        sums[i] = sums[i] + wv * column(g, d, i)
            for n in range(9):
                acc[b, n] = sums[n]
            return carried

        lax.fori_loop(0, BANDS, band, 0)

    def solve(t, passed):
        def band(b, carried):
            def total_of(n):
                total = own_sums[t, b, n]
                return total + got_sums[t, b, n] if passed else total

            fit = []
            explained = None
            for i in range(8):
                total = total_of(i)
                for k in range(i):
                    total = total - low[t, pair(k, i)] * fit[k]
                total = total * low[t, pair(i, i)]
                fit.append(total)
                explained = total * total if i == 0 else explained + total * total
            for i in range(7, -1, -1):
                total = fit[i]
                for k in range(i + 1, 8):
                    total = total - low[t, pair(i, k)] * fit[k]
                total = total * low[t, pair(i, i)]
                fit[i] = total
                res[t, 0, b, i] = total[0:8, :]
                res[t, 1, b, i] = total[8:16, :]
                explained = explained + SCALE * total * total
            ssr = jnp.maximum(total_of(8) - explained, 0.0)
            arsum[b] = arsum[b] + ssr[0:8, :] + ssr[8:16, :]
            ratio = jnp.sqrt(ssr / (gram[t, 0] + SCALE))
            sres[t, 0, b] = ratio[0:8, :]
            sres[t, 1, b] = ratio[8:16, :]
            return carried

        lax.fori_loop(0, BANDS, band, 0)

    def lanes(pz, pc):
        return pl.ds(pl.multiple_of((pz * 2 + pc) * 128, 128), 128)

    def out_copies(t, half, slot, dev):
        return (
            remote(sres.at[t, half], sstage.at[z * 2 + c], ss.at[t, half], sr.at[t, slot], dev),
            remote(res.at[t, half], coef_out.at[:, :, :, lanes(z, c)], cs.at[t, half], cr.at[t, slot], dev),
        )

    def y_results():
        slot = lax.rem(y - turn + 3, 4)
        dev = (x, pix(turn, z, c))
        return (
            remote(sres.at[0], ysres.at[slot], e_s.at[0], e_r.at[slot, 0], dev),
            remote(res.at[0], yres.at[slot], e_s.at[1], e_r.at[slot, 1], dev),
        )

    def y_arrival(slot):
        dev = (x, pix(turn, z, c))
        return (
            remote(sres.at[0], ysres.at[slot], e_s.at[0], e_r.at[slot, 0], dev),
            remote(res.at[0], yres.at[slot], e_s.at[1], e_r.at[slot, 1], dev),
        )

    def turned(i, half):
        dev = (lax.rem(y + i, 4), pix(y, lax.rem(z + 1, 4), half))
        src_score = sres.at[0, half] if i == 0 else ysres.at[i - 1, half]
        src = res.at[0, half] if i == 0 else yres.at[i - 1, half]
        return (
            remote(src_score, sstage.at[z * 2 + c], fs.at[i, half], sr.at[0, c], dev),
            remote(src, coef_out.at[:, :, :, lanes(z, c)], fc.at[i, half], cr.at[0, c], dev),
        )

    def step(s, carried):
        @pl.when(s < STEPS)
        def _():
            t = lax.div(s, PARTS)
            q = lax.rem(s, PARTS)

            @pl.when(jnp.logical_and(t == 0, q > 0))
            def _():
                for i in range(4):
                    first_local(q, i).wait()

            @pl.when(t > 0)
            def _():
                y_local(s, t, q).wait()
                for tp in range(1, 4):
                    y_copy(s, t, q, tp).wait_recv()

            @pl.when(jnp.logical_and(s > 0, t < last))
            def _():
                a_copy(s, t, q).start()
                b_copy(s, t, q).start()

            @pl.when(t == last)
            def _():
                for tp in (2, 1, 3):
                    x_copy(q, tp).start()

            @pl.when(q == 0)
            def _():
                @pl.when(t > 0)
                def _():
                    for tp in range(1, 4):
                        yw_copy(t, tp).wait_recv()

                @pl.when(t < last)
                def _():
                    wa_copy(t).start()
                    wb_copy(t).start()
                    wc_copy(t).start()

                @pl.when(t == last)
                def _():
                    for tp in (2, 1, 3):
                        xw_copy(tp).start()

            nxt = s + PARTS + AHEAD

            @pl.when(nxt < STEPS)
            def _():
                @pl.when(lax.rem(nxt, PARTS) == 0)
                def _():
                    yw_start(lax.div(nxt, PARTS))

                y_start(nxt)

        @pl.when(s >= LAG)
        def _():
            n = s - LAG
            t = lax.div(n, PARTS)
            q = lax.rem(n, PARTS)

            @pl.when(n == 0)
            def _():
                columns()

            @pl.when(q == 0)
            def _():
                own_sums[t] = jnp.zeros((BANDS, 9, 16, 128), F32)

                @pl.when(t < last)
                def _():
                    pass_sums[t] = jnp.zeros((BANDS, 9, 16, 128), F32)
                    wa_copy(t).wait_recv()
                    wd_copy(t).start()
                    wb_copy(t).wait_recv()

                @pl.when(t == last)
                def _():
                    for tp in range(1, 4):
                        xw_copy(tp).wait_recv()

            @pl.when(t < last)
            def _():
                a_copy(n, t, q).wait_recv()
                moments(
                    pass_sums.at[t],
                    [(mid.at[fore_slot, t], midw.at[fore_slot, t], 0), (carry.at[t], carryw.at[t], back)],
                    q,
                )

                @pl.when(q == PARTS - 1)
                def _():
                    sum_copy(t).start()

                b_copy(n, t, q).wait_recv()

            @pl.when(t == last)
            def _():
                for tp in range(1, 4):
                    x_copy(q, tp).wait_recv()
                moments(
                    own_sums.at[t],
                    [(far.at[1, t], farw.at[1, t], 2), (far.at[2 - 2 * c, t], farw.at[2 - 2 * c, t], back)],
                    q,
                )

            moments(
                own_sums.at[t],
                [(mid.at[home, t], midw.at[home, t], 0), (far.at[2 * c, t], farw.at[2 * c, t], fore)],
                q,
            )

            @pl.when(q == PARTS - 2)
            def _():
                @pl.when(t < last)
                def _():
                    wc_copy(t).wait_recv()
                    wd_copy(t).wait_recv()

                factor(t)

                @pl.when(t > 0)
                def _():
                    sum_copy(t - 1).wait_recv()
                    solve(t - 1, True)

                @pl.when(jnp.logical_and(t == 1, turn != y))
                def _():
                    for copy in y_results():
                        copy.start()

                @pl.when(t > 1)
                def _():
                    for half in range(2):
                        dev = (x, pix(y, lax.rem(z + t, 4), half))
                        for copy in out_copies(t - 1, half, c, dev):
                            copy.start()

            @pl.when(jnp.logical_and(n == last * PARTS, turn == y))
            def _():
                for slot in range(3):
                    for copy in y_arrival(slot):
                        copy.wait_recv()
                for i in range(4):
                    for half in range(2):
                        for copy in turned(i, half):
                            copy.start()

        return carried

    lax.fori_loop(0, STEPS + LAG, step, 0)
    solve(last, False)

    twin = (x, pix(y, z, 1 - c))
    arsrc[0] = jnp.sum(arsum[...], axis=1)

    def gather(stage, peers, first):
        copies = [
            remote(arsrc.at[stage], arbuf.at[first + n], as_.at[first + n], ar_.at[first + n], dev)
            for n, dev in enumerate(peers)
        ]
        for copy in copies:
            copy.start()
        return copies

    copies = gather(0, z_peers, 0)
    twin_copies = out_copies(last, 1 - c, 0, twin)
    for copy in twin_copies:
        copy.start()
    own = pltpu.make_async_copy(res.at[last, c], coef_out.at[:, :, :, lanes(z, c)], c_loc)
    own.start()
    sstage[z * 2 + c] = sres[last, c]
    started = list(copies)
    for copy in copies:
        copy.wait_recv()
    total = arsrc[0]
    for n in range(7):
        total = total + arbuf[n]
    arsrc[1] = total
    copies = gather(1, plane_peers, 7)
    started += copies
    for copy in copies:
        copy.wait_recv()
    total = arsrc[1]
    for n in range(15):
        total = total + arbuf[7 + n]
    total = jnp.sum(total, axis=1, keepdims=True)
    inverse = 1.0 / jnp.sqrt(total / total[7:8, :])

    for t in range(last):
        for half in range(2):
            dev = (x, pix(y, lax.rem(z + 1 + t, 4), half))
            for copy in out_copies(t, half, half, dev):
                copy.wait_recv()
                if t > 0:
                    copy.wait_send()
    for copy in twin_copies:
        copy.wait()
    own.wait()
    for b in range(BANDS):
        factor_b = jnp.broadcast_to(inverse[b:b + 1, :], (8, 128))
        for n in range(8):
            score_out[b, :, n * 128:(n + 1) * 128] = sstage[n, b] * factor_b

    for copy in started:
        copy.wait_send()
    for tp in range(1, 4):
        d_remote(tp).wait_send()
        xw_copy(tp).wait_send()

    @pl.when(turn != y)
    def _():
        for copy in y_results():
            copy.wait_send()

    @pl.when(turn == y)
    def _():
        for i in range(4):
            for half in range(2):
                for copy in turned(i, half):
                    copy.wait_send()

    def drain(s, carried):
        t = lax.div(s, PARTS)
        q = lax.rem(s, PARTS)

        @pl.when(t > 0)
        def _():
            for tp in range(1, 4):
                y_copy(s, t, q, tp).wait_send()

        @pl.when(t < last)
        def _():
            a_copy(s, t, q).wait_send()
            b_copy(s, t, q).wait_send()

        @pl.when(t == last)
        def _():
            for tp in range(1, 4):
                x_copy(q, tp).wait_send()

        @pl.when(q == 0)
        def _():
            @pl.when(t > 0)
            def _():
                for tp in range(1, 4):
                    yw_copy(t, tp).wait_send()

            @pl.when(t < last)
            def _():
                for copy in (wa_copy(t), wb_copy(t), wc_copy(t), wd_copy(t), sum_copy(t)):
                    copy.wait_send()

        return carried

    lax.fori_loop(0, STEPS, drain, 0)


def local(stack, quality, days):
    design = jnp.pad(design_matrix(days), ((0, 0), (0, 120)))
    dma = pltpu.SemaphoreType.DMA
    vmem = pltpu.VMEM
    hbm = pl.BlockSpec(memory_space=pltpu.HBM)
    samples = (GROUP, BANDS, 16, 128)
    codes = (GROUP, 16, 128)
    return pl.pallas_call(
        fit_kernel,
        out_shape=(
            jax.ShapeDtypeStruct((BANDS, 8, 8, 1024), F32),
            jax.ShapeDtypeStruct((BANDS, 8, 1024), F32),
        ),
        in_specs=[hbm, hbm, hbm],
        out_specs=(hbm, pl.BlockSpec(memory_space=pltpu.VMEM)),
        scratch_shapes=[
            vmem((4, CHUNKS) + samples, BF16),
            vmem((4, CHUNKS) + codes, BF16),
            vmem((3, CHUNKS) + samples, BF16),
            vmem((3, CHUNKS) + codes, BF16),
            vmem((CHUNKS - 1,) + samples, BF16),
            vmem((CHUNKS - 1,) + codes, BF16),
            vmem((3, CHUNKS) + codes, BF16),
            vmem((GROUP, 256, 128), jnp.int32),
            vmem((4, GROUP, 128), F32),
            vmem((4, GROUP, 8, 8, 128), F32),
            vmem((CHUNKS, BANDS, 9, 16, 128), F32),
            vmem((CHUNKS - 1, BANDS, 9, 16, 128), F32),
            vmem((CHUNKS - 1, BANDS, 9, 16, 128), F32),
            vmem((CHUNKS, 36, 16, 128), F32),
            vmem((CHUNKS, 36, 16, 128), F32),
            vmem((CHUNKS, 2, BANDS, 8, 8, 128), F32),
            vmem((CHUNKS, 2, BANDS, 8, 128), F32),
            vmem((3, 2, BANDS, 8, 8, 128), F32),
            vmem((3, 2, BANDS, 8, 128), F32),
            vmem((8, BANDS, 8, 128), F32),
            vmem((8, 8, 128), F32),
            vmem((2, 8, 128), F32),
            vmem((22, 8, 128), F32),
            dma, dma((STEPS, 4)), dma,
            dma((STEPS, 3)), dma((STEPS, 3)), dma((CHUNKS, 3)), dma((CHUNKS, 3)),
            dma((STEPS,)), dma((STEPS,)), dma((STEPS,)), dma((STEPS,)), dma((PARTS, 3)), dma((PARTS, 3)),
            dma((CHUNKS,)), dma((CHUNKS,)), dma((CHUNKS, 3)), dma((CHUNKS, 3)), dma((CHUNKS,)), dma((CHUNKS,)),
            dma((3,)), dma((3,)), dma((2,)), dma((3, 2)), dma((4, 2)), dma((4, 2)),
            dma((CHUNKS, 2)), dma((CHUNKS, 2)), dma((CHUNKS, 2)), dma((CHUNKS, 2)),
            dma, dma((22,)), dma((22,)),
        ],
        compiler_params=pltpu.CompilerParams(
            collective_id=0, has_side_effects=True, vmem_limit_bytes=48 * 1024 * 1024
        ),
        name="fit",
    )(stack, quality, design)


def solution(mesh):
    return jax.shard_map(
        local,
        mesh=mesh,
        in_specs=(P("date", None, None, "pix"), P("date", None, "pix"), P("date")),
        out_specs=(P(None, None, "pix", "date"), P(None, "pix", "date")),
        check_vma=False,
    )
```

```python
import jax
import jax.numpy as jnp
from jax import lax
from jax.experimental import pallas as pl
from jax.experimental.pallas import tpu as pltpu
from jax.sharding import PartitionSpec as P

MESH = pl.DeviceIdType.MESH
F32 = jnp.float32
BF16 = jnp.bfloat16

BANDS = 7
GROUP = 16
PARTS = 4
DPART = GROUP // PARTS
CHUNKS = 4
STEPS = CHUNKS * PARTS
AHEAD = 7
RAMP = 11
EARLY = 2
LAG = 3
FACTOR_AT = 2
SOLVE_AT = 1
TURN_AT = 14
CHAINED = 3
SCALE = 12.0
PAIRS = [(i, j) for i in range(8) for j in range(i, 8)]


def pair(i, j):
    return PAIRS.index((min(i, j), max(i, j)))


def design_matrix(days):
    moment_t = days.astype(F32)
    columns = [jnp.ones_like(moment_t), (moment_t - 512.0) / 512.0]
    for order in range(1, 4):
        phase = 2.0 * jnp.pi * order * moment_t / 365.25
        columns.append(jnp.cos(phase))
        columns.append(jnp.sin(phase))
    return jnp.stack(columns, 1)


def fit_kernel(
    stack, quality, design, coef_out, score_out,
    mid, midw, far, farw, carry, carryw, wout, qv, dbuf, dfull, own_sums, pass_sums, got_sums,
    gram, low, res, sres, yres, ysres, sstage, arsum, arsrc, arbuf,
    q_sem, l_sem, d_loc, ys, yr, yws, ywr, a_s, a_r, b_s, b_r, xs, xr, wa_s, wa_r, ws, wr, sm_s, sm_r,
    ds_, dr_, e_s, e_r, fc, fs, cs, cr, ss, sr, c_loc, as_, ar_,
):
    x = lax.axis_index("date")
    p = lax.axis_index("pix")
    y = lax.div(p, 8)
    z = lax.rem(lax.div(p, 2), 4)
    c = lax.rem(p, 2)
    last = CHUNKS - 1

    def pix(py, pz, pc):
        return (py * 4 + pz) * 2 + pc

    def right(n):
        return (lax.rem(x + n, 4), p)

    fore = 1 + 2 * c
    back = 3 - 2 * c
    fore_dev = right(fore)
    back_dev = right(back)
    home = lax.rem(x - y + 4, 4)
    fore_slot = lax.rem(x + fore - y + 4, 4)
    back_slot = lax.rem(x + back - y + 4, 4)
    far_slot = lax.rem(x + 2 - y + 4, 4)
    turn = lax.rem(x + 2 * c, 4)

    y_peers = [(x, pix(lax.rem(y + t, 4), z, c)) for t in range(1, 4)]
    x_peers = [right(t) for t in range(1, 4)]
    plane_peers = [
        (lax.rem(x + n // 4, 4), pix(lax.rem(y + n % 4, 4), z, c)) for n in range(1, 16)
    ]
    z_peers = [
        (x, pix(y, lax.rem(z + e // 2, 4), lax.rem(c + e % 2, 2))) for e in range(1, 8)
    ]

    def remote(src, dst, send, recv, dev):
        return pltpu.make_async_remote_copy(
            src_ref=src, dst_ref=dst, send_sem=send, recv_sem=recv,
            device_id=dev, device_id_type=MESH,
        )

    def dates(q):
        return pl.ds(q * DPART, DPART)

    def row_z(t):
        return lax.rem(z + (1 + t) * (3 - 2 * c), 4)

    def chunk_row(ry, t):
        return pl.multiple_of(ry * 64 + row_z(t) * 16, 16)

    def first_local(q, i):
        ry = lax.rem(y + i + 2 * c, 4)
        return pltpu.make_async_copy(
            stack.at[dates(q), :, pl.ds(chunk_row(ry, 0), 16), :],
            mid.at[i, 0, dates(q)],
            l_sem.at[q, i],
        )

    def y_local(s, t, q):
        return pltpu.make_async_copy(
            stack.at[dates(q), :, pl.ds(chunk_row(y, t), 16), :],
            mid.at[0, t, dates(q)],
            l_sem.at[s, 0],
        )

    def y_copy(s, t, q, tp):
        ry = lax.rem(y + tp, 4)
        return remote(
            stack.at[dates(q), :, pl.ds(chunk_row(ry, t), 16), :],
            mid.at[4 - tp, t, dates(q)],
            ys.at[s, tp - 1], yr.at[s, 3 - tp], y_peers[tp - 1],
        )

    def yw_copy(t, tp):
        return remote(
            wout.at[tp - 1, t], midw.at[4 - tp, t],
            yws.at[t, tp - 1], ywr.at[t, 3 - tp], y_peers[tp - 1],
        )

    def a_copy(s, t, q):
        return remote(mid.at[far_slot, t, dates(q)], carry.at[t, dates(q)], a_s.at[s], a_r.at[s], fore_dev)

    def b_copy(s, t, q):
        return remote(mid.at[back_slot, t, dates(q)], far.at[2 * c, t, dates(q)], b_s.at[s], b_r.at[s], back_dev)

    def x_copy(s, t, q, tp):
        i = lax.rem(x + tp - y + 4, 4)
        return remote(
            mid.at[i, t, dates(q)], far.at[3 - tp, t, dates(q)],
            xs.at[s, tp - 1], xr.at[s, 3 - tp], x_peers[tp - 1],
        )

    def xw_copy(t, tp):
        i = lax.rem(x + tp - y + 4, 4)
        return remote(
            midw.at[i, t], farw.at[3 - tp, t],
            ws.at[t, tp - 1], wr.at[t, 3 - tp], x_peers[tp - 1],
        )

    def wa_copy(t):
        return remote(midw.at[far_slot, t], carryw.at[t], wa_s.at[t], wa_r.at[t], fore_dev)

    def wb_copy(t):
        return remote(midw.at[back_slot, t], farw.at[2 * c, t], ws.at[t, 0], wr.at[t, 2 * c], back_dev)

    def wc_copy(t):
        return remote(midw.at[fore_slot, t], farw.at[2 - 2 * c, t], ws.at[t, 1], wr.at[t, 2 - 2 * c], fore_dev)

    def wd_copy(t):
        return remote(carryw.at[t], farw.at[1, t], ws.at[t, 2], wr.at[t, 1], fore_dev)

    def sum_copy(t):
        return remote(pass_sums.at[t], got_sums.at[t], sm_s.at[t], sm_r.at[t], fore_dev)

    def d_remote(tp):
        return remote(design, dbuf.at[4 - tp], ds_.at[tp - 1], dr_.at[3 - tp], x_peers[tp - 1])

    def y_start(s):
        t = lax.div(s, PARTS)
        q = lax.rem(s, PARTS)
        for tp in (2, 1, 3):
            y_copy(s, t, q, tp).start()
        y_local(s, t, q).start()

    def yw_start(t):
        for tp in (2, 1, 3):
            yw_copy(t, tp).start()

    for i in range(4):
        first_local(0, i).start()
    q_copy = pltpu.make_async_copy(quality, qv, q_sem)
    q_copy.start()
    for q in range(1, PARTS):
        for i in range(4):
            first_local(q, i).start()
    d_copy = pltpu.make_async_copy(design, dbuf.at[0], d_loc)
    d_copy.start()

    barrier = pltpu.get_barrier_semaphore()
    for dev in y_peers + x_peers + z_peers:
        pl.semaphore_signal(barrier, inc=1, device_id=dev, device_id_type=MESH)
    pl.semaphore_wait(barrier, 13)

    def first_start(q):
        for i in range(4):
            first_local(q, i).wait()
        a_copy(q, 0, q).start()
        b_copy(q, 0, q).start()

    y_start(PARTS)
    first_start(0)
    for q in range(1, 1 + PARTS // 4):
        first_start(q)
    for tp in range(1, 4):
        d_remote(tp).start()

    def x_codes(t):
        wa_copy(t).start()
        wb_copy(t).start()
        wc_copy(t).start()

    q_copy.wait()

    def encode(n, carried):
        t = lax.div(n, 4)
        tp = lax.rem(n, 4)
        ry = lax.rem(y + tp + jnp.where(t == 0, 2 * c, 0), 4)
        bits = qv[:, pl.ds(chunk_row(ry, t), 16), :]
        level = jnp.bitwise_and(jnp.right_shift(bits, 8), 3)
        clear = jnp.bitwise_and(bits, 8) == 0
        code = jnp.where(level == 0, 12.0, jnp.where(level == 1, 6.0, jnp.where(level == 2, 4.0, 3.0)))
        code = jnp.where(clear, code, 0.0).astype(BF16)
        kept = jnp.logical_or(t == 0, tp == 0)

        @pl.when(kept)
        def _():
            midw[tp, t] = code

        @pl.when(jnp.logical_not(kept))
        def _():
            wout[tp - 1, t] = code

        return carried

    lax.fori_loop(0, 4 * CHUNKS, encode, 0)
    yw_start(1)
    x_codes(0)
    for q in range(1 + PARTS // 4, PARTS):
        first_start(q)
    for s in range(PARTS + 1, PARTS + AHEAD):
        if s % PARTS == 0:
            yw_start(s // PARTS)
        y_start(s)
    arsum[...] = jnp.zeros_like(arsum)

    def column(g, d, i):
        v = dfull[g, d, i]
        return jnp.concatenate([v, v], 0)

    def columns():
        d_copy.wait()
        for tp in range(1, 4):
            d_remote(tp).wait_recv()

        def spread(n, carried):
            g = lax.div(n, GROUP)
            d = lax.rem(n, GROUP)
            row = dbuf[g, pl.ds(d, 1), :]
            for i in range(8):
                dfull[g, d, i] = jnp.broadcast_to(row[:, i:i + 1], (8, 128))
            return carried

        lax.fori_loop(0, 4 * GROUP, spread, 0)

    def factor(t):
        codes = [midw.at[home, t]] + [farw.at[j, t] for j in range(3)]
        for rows in ((0, 1), (2, 3), (4, 5, 6, 7)):
            wanted = [(i, j) for i in rows for j in range(i, 8)]

            def add(d, sums, rows=rows, wanted=wanted):
                sums = list(sums)
                for g in range(4):
                    w = codes[g][d].astype(F32)
                    cols = {k: column(g, d, k) for k in range(rows[0], 8)}
                    for i in rows:
                        wd = w if i == 0 else w * cols[i]
                        for j in range(i, 8):
                            n = wanted.index((i, j))
                            sums[n] = sums[n] + (wd if j == 0 else wd * cols[j])
                return tuple(sums)

            sums = lax.fori_loop(
                0, GROUP, add, tuple(jnp.zeros((16, 128), F32) for _ in wanted)
            )
            for n, (i, j) in enumerate(wanted):
                gram[t, pair(i, j)] = sums[n]
        for half in (0, 8):
            lower = {}
            for j in range(8):
                total = gram[t, pair(j, j), half:half + 8, :] + SCALE
                for k in range(j):
                    total = total - lower[j, k] * lower[j, k]
                inverse = 1.0 / jnp.sqrt(total)
                low[t, pair(j, j), half:half + 8, :] = inverse
                for i in range(j + 1, 8):
                    total = gram[t, pair(j, i), half:half + 8, :]
                    for k in range(j):
                        total = total - lower[i, k] * lower[j, k]
                    lower[i, j] = total * inverse
                    low[t, pair(j, i), half:half + 8, :] = lower[i, j]
        arsum[7] = arsum[7] + gram[t, 0, 0:8, :] + gram[t, 0, 8:16, :]

    def moments(acc, refs, q):
        def band(b, carried):
            sums = [acc[b, n] for n in range(9)]
            for values, codes, g in refs:
                for dd in range(DPART):
                    d = q * DPART + dd
                    v = values[d, b].astype(F32)
                    wv = codes[d].astype(F32) * v
                    sums[8] = sums[8] + wv * v
                    sums[0] = sums[0] + wv
                    for i in range(1, 8):
                        sums[i] = sums[i] + wv * column(g, d, i)
            for n in range(9):
                acc[b, n] = sums[n]
            return carried

        lax.fori_loop(0, BANDS, band, 0)

    def solve(t, passed):
        def band(b, carried):
            def total_of(n):
                total = own_sums[t, b, n]
                return total + got_sums[t, b, n] if passed else total

            fit = []
            explained = None
            for i in range(8):
                total = total_of(i)
                for k in range(i):
                    total = total - low[t, pair(k, i)] * fit[k]
                total = total * low[t, pair(i, i)]
                fit.append(total)
                explained = total * total if i == 0 else explained + total * total
            for i in range(7, -1, -1):
                total = fit[i]
                for k in range(i + 1, 8):
                    total = total - low[t, pair(i, k)] * fit[k]
                total = total * low[t, pair(i, i)]
                fit[i] = total
                res[t, 0, b, i] = total[0:8, :]
                res[t, 1, b, i] = total[8:16, :]
                explained = explained + SCALE * total * total
            ssr = jnp.maximum(total_of(8) - explained, 0.0)
            arsum[b] = arsum[b] + ssr[0:8, :] + ssr[8:16, :]
            ratio = jnp.sqrt(ssr / (gram[t, 0] + SCALE))
            sres[t, 0, b] = ratio[0:8, :]
            sres[t, 1, b] = ratio[8:16, :]
            return carried

        lax.fori_loop(0, BANDS, band, 0)

    def lanes(pz, pc):
        return pl.ds(pl.multiple_of((pz * 2 + pc) * 128, 128), 128)

    def out_copies(t, half, slot, dev):
        return (
            remote(sres.at[t, half], sstage.at[z * 2 + c], ss.at[t, half], sr.at[t, slot], dev),
            remote(res.at[t, half], coef_out.at[:, :, :, lanes(z, c)], cs.at[t, half], cr.at[t, slot], dev),
        )

    def y_results():
        slot = lax.rem(y - turn + 3, 4)
        dev = (x, pix(turn, z, c))
        return (
            remote(sres.at[0], ysres.at[slot], e_s.at[0], e_r.at[slot, 0], dev),
            remote(res.at[0], yres.at[slot], e_s.at[1], e_r.at[slot, 1], dev),
        )

    def y_arrival(slot):
        dev = (x, pix(turn, z, c))
        return (
            remote(sres.at[0], ysres.at[slot], e_s.at[0], e_r.at[slot, 0], dev),
            remote(res.at[0], yres.at[slot], e_s.at[1], e_r.at[slot, 1], dev),
        )

    def turned(i, half):
        dev = (lax.rem(y + i, 4), pix(y, row_z(0), half))
        src_score = sres.at[0, half] if i == 0 else ysres.at[i - 1, half]
        src = res.at[0, half] if i == 0 else yres.at[i - 1, half]
        return (
            remote(src_score, sstage.at[z * 2 + c], fs.at[i, half], sr.at[0, c], dev),
            remote(src, coef_out.at[:, :, :, lanes(z, c)], fc.at[i, half], cr.at[0, c], dev),
        )

    def due(s):
        ramp = s - LAG + jnp.maximum(s - RAMP, 0)
        return jnp.maximum(jnp.minimum(s - EARLY, PARTS - 1), jnp.minimum(ramp, s - 1))

    def use(n, carried):
        t = lax.div(n, PARTS)
        q = lax.rem(n, PARTS)

        @pl.when(n == 0)
        def _():
            columns()

        @pl.when(q == 0)
        def _():
            own_sums[t] = jnp.zeros((BANDS, 9, 16, 128), F32)

            @pl.when(t < CHAINED)
            def _():
                pass_sums[t] = jnp.zeros((BANDS, 9, 16, 128), F32)
                wa_copy(t).wait_recv()
                wd_copy(t).start()
                wb_copy(t).wait_recv()

            @pl.when(t >= CHAINED)
            def _():
                for tp in range(1, 4):
                    xw_copy(t, tp).wait_recv()

        @pl.when(t < CHAINED)
        def _():
            a_copy(n, t, q).wait_recv()
            moments(
                pass_sums.at[t],
                [(mid.at[fore_slot, t], midw.at[fore_slot, t], 0), (carry.at[t], carryw.at[t], back)],
                q,
            )

            @pl.when(q == PARTS - 1)
            def _():
                sum_copy(t).start()

            b_copy(n, t, q).wait_recv()

        @pl.when(t >= CHAINED)
        def _():
            for tp in range(1, 4):
                x_copy(n, t, q, tp).wait_recv()
            moments(
                own_sums.at[t],
                [(far.at[1, t], farw.at[1, t], 2), (far.at[2 - 2 * c, t], farw.at[2 - 2 * c, t], back)],
                q,
            )

        moments(
            own_sums.at[t],
            [(mid.at[home, t], midw.at[home, t], 0), (far.at[2 * c, t], farw.at[2 * c, t], fore)],
            q,
        )

        @pl.when(q == FACTOR_AT)
        def _():
            @pl.when(t < CHAINED)
            def _():
                wc_copy(t).wait_recv()
                wd_copy(t).wait_recv()

            factor(t)

        def send_results(done):
            for half in range(2):
                dev = (x, pix(y, row_z(done), half))
                for copy in out_copies(done, half, c, dev):
                    copy.start()

        @pl.when(jnp.logical_and(q == SOLVE_AT, jnp.logical_and(t > 0, t <= CHAINED)))
        def _():
            sum_copy(t - 1).wait_recv()
            solve(t - 1, True)

            @pl.when(jnp.logical_and(t == 1, turn != y))
            def _():
                for copy in y_results():
                    copy.start()

            @pl.when(t > 1)
            def _():
                send_results(t - 1)

        @pl.when(jnp.logical_and(q == PARTS - 1, t >= CHAINED))
        def _():
            solve(t, False)

            @pl.when(t < last)
            def _():
                send_results(t)

        @pl.when(jnp.logical_and(n == TURN_AT, turn == y))
        def _():
            for slot in range(3):
                for copy in y_arrival(slot):
                    copy.wait_recv()
            for i in range(4):
                for half in range(2):
                    for copy in turned(i, half):
                        copy.start()

        return carried

    def step(s, carried):
        @pl.when(jnp.logical_and(s >= PARTS, s < STEPS))
        def _():
            t = lax.div(s, PARTS)
            q = lax.rem(s, PARTS)
            y_local(s, t, q).wait()
            for tp in range(1, 4):
                y_copy(s, t, q, tp).wait_recv()

            @pl.when(t < CHAINED)
            def _():
                a_copy(s, t, q).start()
                b_copy(s, t, q).start()

            @pl.when(t >= CHAINED)
            def _():
                for tp in (2, 1, 3):
                    x_copy(s, t, q, tp).start()

            @pl.when(q == 0)
            def _():
                for tp in range(1, 4):
                    yw_copy(t, tp).wait_recv()

                @pl.when(t < CHAINED)
                def _():
                    x_codes(t)

                @pl.when(t >= CHAINED)
                def _():
                    for tp in (2, 1, 3):
                        xw_copy(t, tp).start()

            nxt = s + AHEAD

            @pl.when(nxt < STEPS)
            def _():
                @pl.when(lax.rem(nxt, PARTS) == 0)
                def _():
                    yw_start(lax.div(nxt, PARTS))

                y_start(nxt)

        lax.fori_loop(due(s - 1) + 1, due(s) + 1, use, 0)
        return carried

    lax.fori_loop(EARLY, STEPS + 1, step, 0)

    twin = (x, pix(y, z, 1 - c))
    arsrc[0] = jnp.sum(arsum[...], axis=1)

    def gather(stage, peers, first):
        copies = [
            remote(arsrc.at[stage], arbuf.at[first + n], as_.at[first + n], ar_.at[first + n], dev)
            for n, dev in enumerate(peers)
        ]
        for copy in copies:
            copy.start()
        return copies

    copies = gather(0, z_peers, 0)
    twin_copies = out_copies(last, 1 - c, 0, twin)
    for copy in twin_copies:
        copy.start()
    own = pltpu.make_async_copy(res.at[last, c], coef_out.at[:, :, :, lanes(z, c)], c_loc)
    own.start()
    sstage[z * 2 + c] = sres[last, c]
    started = list(copies)
    for copy in copies:
        copy.wait_recv()
    total = arsrc[0]
    for n in range(7):
        total = total + arbuf[n]
    arsrc[1] = total
    copies = gather(1, plane_peers, 7)
    started += copies
    for copy in copies:
        copy.wait_recv()
    total = arsrc[1]
    for n in range(15):
        total = total + arbuf[7 + n]
    total = jnp.sum(total, axis=1, keepdims=True)
    inverse = 1.0 / jnp.sqrt(total / total[7:8, :])

    for t in range(last):
        for half in range(2):
            dev = (x, pix(y, row_z(t), half))
            for copy in out_copies(t, half, half, dev):
                copy.wait_recv()
                if t > 0:
                    copy.wait_send()
    for copy in twin_copies:
        copy.wait()
    own.wait()
    for b in range(BANDS):
        factor_b = jnp.broadcast_to(inverse[b:b + 1, :], (8, 128))
        for n in range(8):
            score_out[b, :, n * 128:(n + 1) * 128] = sstage[n, b] * factor_b

    for copy in started:
        copy.wait_send()
    for tp in range(1, 4):
        d_remote(tp).wait_send()

    @pl.when(turn != y)
    def _():
        for copy in y_results():
            copy.wait_send()

    @pl.when(turn == y)
    def _():
        for i in range(4):
            for half in range(2):
                for copy in turned(i, half):
                    copy.wait_send()

    def drain(s, carried):
        t = lax.div(s, PARTS)
        q = lax.rem(s, PARTS)

        @pl.when(t > 0)
        def _():
            for tp in range(1, 4):
                y_copy(s, t, q, tp).wait_send()

        @pl.when(t < CHAINED)
        def _():
            a_copy(s, t, q).wait_send()
            b_copy(s, t, q).wait_send()

        @pl.when(t >= CHAINED)
        def _():
            for tp in range(1, 4):
                x_copy(s, t, q, tp).wait_send()

        @pl.when(q == 0)
        def _():
            @pl.when(t > 0)
            def _():
                for tp in range(1, 4):
                    yw_copy(t, tp).wait_send()

            @pl.when(t < CHAINED)
            def _():
                for copy in (wa_copy(t), wb_copy(t), wc_copy(t), wd_copy(t), sum_copy(t)):
                    copy.wait_send()

            @pl.when(t >= CHAINED)
            def _():
                for tp in range(1, 4):
                    xw_copy(t, tp).wait_send()

        return carried

    lax.fori_loop(0, STEPS, drain, 0)


def local(stack, quality, days):
    design = jnp.pad(design_matrix(days), ((0, 0), (0, 120)))
    dma = pltpu.SemaphoreType.DMA
    vmem = pltpu.VMEM
    hbm = pl.BlockSpec(memory_space=pltpu.HBM)
    samples = (GROUP, BANDS, 16, 128)
    codes = (GROUP, 16, 128)
    return pl.pallas_call(
        fit_kernel,
        out_shape=(
            jax.ShapeDtypeStruct((BANDS, 8, 8, 1024), F32),
            jax.ShapeDtypeStruct((BANDS, 8, 1024), F32),
        ),
        in_specs=[hbm, hbm, hbm],
        out_specs=(hbm, pl.BlockSpec(memory_space=pltpu.VMEM)),
        scratch_shapes=[
            vmem((4, CHUNKS) + samples, BF16),
            vmem((4, CHUNKS) + codes, BF16),
            vmem((3, CHUNKS) + samples, BF16),
            vmem((3, CHUNKS) + codes, BF16),
            vmem((CHAINED,) + samples, BF16),
            vmem((CHAINED,) + codes, BF16),
            vmem((3, CHUNKS) + codes, BF16),
            vmem((GROUP, 256, 128), jnp.int32),
            vmem((4, GROUP, 128), F32),
            vmem((4, GROUP, 8, 8, 128), F32),
            vmem((CHUNKS, BANDS, 9, 16, 128), F32),
            vmem((CHAINED, BANDS, 9, 16, 128), F32),
            vmem((CHAINED, BANDS, 9, 16, 128), F32),
            vmem((CHUNKS, 36, 16, 128), F32),
            vmem((CHUNKS, 36, 16, 128), F32),
            vmem((CHUNKS, 2, BANDS, 8, 8, 128), F32),
            vmem((CHUNKS, 2, BANDS, 8, 128), F32),
            vmem((3, 2, BANDS, 8, 8, 128), F32),
            vmem((3, 2, BANDS, 8, 128), F32),
            vmem((8, BANDS, 8, 128), F32),
            vmem((8, 8, 128), F32),
            vmem((2, 8, 128), F32),
            vmem((22, 8, 128), F32),
            dma, dma((STEPS, 4)), dma,
            dma((STEPS, 3)), dma((STEPS, 3)), dma((CHUNKS, 3)), dma((CHUNKS, 3)),
            dma((STEPS,)), dma((STEPS,)), dma((STEPS,)), dma((STEPS,)), dma((STEPS, 3)), dma((STEPS, 3)),
            dma((CHUNKS,)), dma((CHUNKS,)), dma((CHUNKS, 3)), dma((CHUNKS, 3)), dma((CHUNKS,)), dma((CHUNKS,)),
            dma((3,)), dma((3,)), dma((2,)), dma((3, 2)), dma((4, 2)), dma((4, 2)),
            dma((CHUNKS, 2)), dma((CHUNKS, 2)), dma((CHUNKS, 2)), dma((CHUNKS, 2)),
            dma, dma((22,)), dma((22,)),
        ],
        compiler_params=pltpu.CompilerParams(
            collective_id=0, has_side_effects=True, vmem_limit_bytes=48 * 1024 * 1024
        ),
        name="fit",
    )(stack, quality, design)


def solution(mesh):
    return jax.shard_map(
        local,
        mesh=mesh,
        in_specs=(P("date", None, None, "pix"), P("date", None, "pix"), P("date")),
        out_specs=(P(None, None, "pix", "date"), P(None, "pix", "date")),
        check_vma=False,
    )
```

```python
import jax
import jax.numpy as jnp
from jax import lax
from jax.experimental import pallas as pl
from jax.experimental.pallas import tpu as pltpu
from jax.sharding import PartitionSpec as P

MESH = pl.DeviceIdType.MESH
F32 = jnp.float32
BF16 = jnp.bfloat16

BANDS = 7
GROUP = 16
PARTS = 4
DPART = GROUP // PARTS
CHUNKS = 4
STEPS = CHUNKS * PARTS
AHEAD = 7
RAMP = 11
EARLY = 2
LAG = 3
FACTOR_AT = 2
SOLVE_AT = 1
TURN_AT = 14
CHAINED = 3
SCALE = 12.0
PAIRS = [(i, j) for i in range(8) for j in range(i, 8)]


def pair(i, j):
    return PAIRS.index((min(i, j), max(i, j)))


def design_matrix(days):
    moment_t = days.astype(F32)
    lane = lax.broadcasted_iota(jnp.int32, (GROUP, 128), 1)
    rate = jnp.where(lane < 4, 2.0 * jnp.pi, jnp.where(lane < 6, 4.0 * jnp.pi, 6.0 * jnp.pi)).astype(F32)
    phase = rate * moment_t / 365.25
    wave = jnp.where(jnp.bitwise_and(lane, 1) == 0, jnp.cos(phase), jnp.sin(phase))
    return jnp.where(lane == 0, 1.0, jnp.where(lane == 1, (moment_t - 512.0) / 512.0, wave))


def fit_kernel(
    stack, quality, design, coef_out, score_out,
    mid, midw, far, farw, carry, carryw, wout, qv, dbuf, dfull, own_sums, pass_sums, got_sums,
    gram, low, res, sres, yres, ysres, sstage, arsum, arsrc, arbuf,
    q_sem, l_sem, d_loc, ys, yr, yws, ywr, a_s, a_r, b_s, b_r, xs, xr, wa_s, wa_r, ws, wr, sm_s, sm_r,
    ds_, dr_, e_s, e_r, fc, fs, cs, cr, ss, sr, c_loc, as_, ar_,
):
    x = lax.axis_index("date")
    p = lax.axis_index("pix")
    y = lax.div(p, 8)
    z = lax.rem(lax.div(p, 2), 4)
    c = lax.rem(p, 2)
    last = CHUNKS - 1

    def pix(py, pz, pc):
        return (py * 4 + pz) * 2 + pc

    def right(n):
        return (lax.rem(x + n, 4), p)

    fore = 1 + 2 * c
    back = 3 - 2 * c
    fore_dev = right(fore)
    back_dev = right(back)
    home = lax.rem(x - y + 4, 4)
    fore_slot = lax.rem(x + fore - y + 4, 4)
    back_slot = lax.rem(x + back - y + 4, 4)
    far_slot = lax.rem(x + 2 - y + 4, 4)
    turn = lax.rem(x + 2 * c, 4)

    y_peers = [(x, pix(lax.rem(y + t, 4), z, c)) for t in range(1, 4)]
    x_peers = [right(t) for t in range(1, 4)]
    plane_peers = [
        (lax.rem(x + n // 4, 4), pix(lax.rem(y + n % 4, 4), z, c)) for n in range(1, 16)
    ]
    z_peers = [
        (x, pix(y, lax.rem(z + e // 2, 4), lax.rem(c + e % 2, 2))) for e in range(1, 8)
    ]

    def remote(src, dst, send, recv, dev):
        return pltpu.make_async_remote_copy(
            src_ref=src, dst_ref=dst, send_sem=send, recv_sem=recv,
            device_id=dev, device_id_type=MESH,
        )

    def dates(q):
        return pl.ds(q * DPART, DPART)

    def row_z(t):
        return lax.rem(z + (1 + t) * (3 - 2 * c), 4)

    def chunk_row(ry, t):
        return pl.multiple_of(ry * 64 + row_z(t) * 16, 16)

    def first_local(q, i):
        ry = lax.rem(y + i + 2 * c, 4)
        return pltpu.make_async_copy(
            stack.at[dates(q), :, pl.ds(chunk_row(ry, 0), 16), :],
            mid.at[i, 0, dates(q)],
            l_sem.at[q, i],
        )

    def y_local(s, t, q):
        return pltpu.make_async_copy(
            stack.at[dates(q), :, pl.ds(chunk_row(y, t), 16), :],
            mid.at[0, t, dates(q)],
            l_sem.at[s, 0],
        )

    def y_copy(s, t, q, tp):
        ry = lax.rem(y + tp, 4)
        return remote(
            stack.at[dates(q), :, pl.ds(chunk_row(ry, t), 16), :],
            mid.at[4 - tp, t, dates(q)],
            ys.at[s, tp - 1], yr.at[s, 3 - tp], y_peers[tp - 1],
        )

    def yw_copy(t, tp):
        return remote(
            wout.at[tp - 1, t], midw.at[4 - tp, t],
            yws.at[t, tp - 1], ywr.at[t, 3 - tp], y_peers[tp - 1],
        )

    def a_copy(s, t, q):
        return remote(mid.at[far_slot, t, dates(q)], carry.at[t, dates(q)], a_s.at[s], a_r.at[s], fore_dev)

    def b_copy(s, t, q):
        return remote(mid.at[back_slot, t, dates(q)], far.at[2 * c, t, dates(q)], b_s.at[s], b_r.at[s], back_dev)

    def x_copy(s, t, q, tp):
        i = lax.rem(x + tp - y + 4, 4)
        return remote(
            mid.at[i, t, dates(q)], far.at[3 - tp, t, dates(q)],
            xs.at[s, tp - 1], xr.at[s, 3 - tp], x_peers[tp - 1],
        )

    def xw_copy(t, tp):
        i = lax.rem(x + tp - y + 4, 4)
        return remote(
            midw.at[i, t], farw.at[3 - tp, t],
            ws.at[t, tp - 1], wr.at[t, 3 - tp], x_peers[tp - 1],
        )

    def wa_copy(t):
        return remote(midw.at[far_slot, t], carryw.at[t], wa_s.at[t], wa_r.at[t], fore_dev)

    def wb_copy(t):
        return remote(midw.at[back_slot, t], farw.at[2 * c, t], ws.at[t, 0], wr.at[t, 2 * c], back_dev)

    def wc_copy(t):
        return remote(midw.at[fore_slot, t], farw.at[2 - 2 * c, t], ws.at[t, 1], wr.at[t, 2 - 2 * c], fore_dev)

    def wd_copy(t):
        return remote(carryw.at[t], farw.at[1, t], ws.at[t, 2], wr.at[t, 1], fore_dev)

    def sum_copy(t):
        return remote(pass_sums.at[t], got_sums.at[t], sm_s.at[t], sm_r.at[t], fore_dev)

    def d_remote(tp):
        return remote(design, dbuf.at[4 - tp], ds_.at[tp - 1], dr_.at[3 - tp], x_peers[tp - 1])

    def y_start(s):
        t = lax.div(s, PARTS)
        q = lax.rem(s, PARTS)
        for tp in (2, 1, 3):
            y_copy(s, t, q, tp).start()
        y_local(s, t, q).start()

    def yw_start(t):
        for tp in (2, 1, 3):
            yw_copy(t, tp).start()

    for i in range(4):
        first_local(0, i).start()
    q_copy = pltpu.make_async_copy(quality, qv, q_sem)
    q_copy.start()
    for q in range(1, PARTS):
        for i in range(4):
            first_local(q, i).start()
    d_copy = pltpu.make_async_copy(design, dbuf.at[0], d_loc)
    d_copy.start()

    barrier = pltpu.get_barrier_semaphore()
    for dev in y_peers + x_peers + z_peers:
        pl.semaphore_signal(barrier, inc=1, device_id=dev, device_id_type=MESH)
    pl.semaphore_wait(barrier, 13)

    def first_start(q):
        for i in range(4):
            first_local(q, i).wait()
        a_copy(q, 0, q).start()
        b_copy(q, 0, q).start()

    y_start(PARTS)
    first_start(0)
    for q in range(1, 1 + PARTS // 4):
        first_start(q)
    for tp in range(1, 4):
        d_remote(tp).start()

    def x_codes(t):
        wa_copy(t).start()
        wb_copy(t).start()
        wc_copy(t).start()

    q_copy.wait()

    def encode(n, carried):
        t = lax.div(n, 4)
        tp = lax.rem(n, 4)
        ry = lax.rem(y + tp + jnp.where(t == 0, 2 * c, 0), 4)
        bits = qv[:, pl.ds(chunk_row(ry, t), 16), :]
        level = jnp.bitwise_and(jnp.right_shift(bits, 8), 3)
        clear = jnp.bitwise_and(bits, 8) == 0
        code = jnp.where(level == 0, 12.0, jnp.where(level == 1, 6.0, jnp.where(level == 2, 4.0, 3.0)))
        code = jnp.where(clear, code, 0.0).astype(BF16)
        kept = jnp.logical_or(t == 0, tp == 0)

        @pl.when(kept)
        def _():
            midw[tp, t] = code

        @pl.when(jnp.logical_not(kept))
        def _():
            wout[tp - 1, t] = code

        return carried

    lax.fori_loop(0, 4 * CHUNKS, encode, 0)
    yw_start(1)
    x_codes(0)
    for q in range(1 + PARTS // 4, PARTS):
        first_start(q)
    for s in range(PARTS + 1, PARTS + AHEAD):
        if s % PARTS == 0:
            yw_start(s // PARTS)
        y_start(s)
    arsum[...] = jnp.zeros_like(arsum)

    def column(g, d, i):
        v = dfull[g, d, i]
        return jnp.concatenate([v, v], 0)

    def columns():
        d_copy.wait()
        for tp in range(1, 4):
            d_remote(tp).wait_recv()

        def spread(n, carried):
            g = lax.div(n, GROUP)
            d = lax.rem(n, GROUP)
            row = dbuf[g, pl.ds(d, 1), :]
            for i in range(8):
                dfull[g, d, i] = jnp.broadcast_to(row[:, i:i + 1], (8, 128))
            return carried

        lax.fori_loop(0, 4 * GROUP, spread, 0)

    def factor(t):
        codes = [midw.at[home, t]] + [farw.at[j, t] for j in range(3)]
        for rows in ((0, 1), (2, 3), (4, 5, 6, 7)):
            wanted = [(i, j) for i in rows for j in range(i, 8)]

            def add(d, sums, rows=rows, wanted=wanted):
                sums = list(sums)
                for g in range(4):
                    w = codes[g][d].astype(F32)
                    cols = {k: column(g, d, k) for k in range(rows[0], 8)}
                    for i in rows:
                        wd = w if i == 0 else w * cols[i]
                        for j in range(i, 8):
                            n = wanted.index((i, j))
                            sums[n] = sums[n] + (wd if j == 0 else wd * cols[j])
                return tuple(sums)

            sums = lax.fori_loop(
                0, GROUP, add, tuple(jnp.zeros((16, 128), F32) for _ in wanted)
            )
            for n, (i, j) in enumerate(wanted):
                gram[t, pair(i, j)] = sums[n]
        for half in (0, 8):
            lower = {}
            for j in range(8):
                total = gram[t, pair(j, j), half:half + 8, :] + SCALE
                for k in range(j):
                    total = total - lower[j, k] * lower[j, k]
                inverse = 1.0 / jnp.sqrt(total)
                low[t, pair(j, j), half:half + 8, :] = inverse
                for i in range(j + 1, 8):
                    total = gram[t, pair(j, i), half:half + 8, :]
                    for k in range(j):
                        total = total - lower[i, k] * lower[j, k]
                    lower[i, j] = total * inverse
                    low[t, pair(j, i), half:half + 8, :] = lower[i, j]
        arsum[7] = arsum[7] + gram[t, 0, 0:8, :] + gram[t, 0, 8:16, :]

    def moments(acc, refs, q):
        def band(b, carried):
            sums = [acc[b, n] for n in range(9)]
            for values, codes, g in refs:
                for dd in range(DPART):
                    d = q * DPART + dd
                    v = values[d, b].astype(F32)
                    wv = codes[d].astype(F32) * v
                    sums[8] = sums[8] + wv * v
                    sums[0] = sums[0] + wv
                    for i in range(1, 8):
                        sums[i] = sums[i] + wv * column(g, d, i)
            for n in range(9):
                acc[b, n] = sums[n]
            return carried

        lax.fori_loop(0, BANDS, band, 0)

    def solve(t, passed):
        def band(b, carried):
            def total_of(n):
                total = own_sums[t, b, n]
                return total + got_sums[t, b, n] if passed else total

            fit = []
            explained = None
            for i in range(8):
                total = total_of(i)
                for k in range(i):
                    total = total - low[t, pair(k, i)] * fit[k]
                total = total * low[t, pair(i, i)]
                fit.append(total)
                explained = total * total if i == 0 else explained + total * total
            for i in range(7, -1, -1):
                total = fit[i]
                for k in range(i + 1, 8):
                    total = total - low[t, pair(i, k)] * fit[k]
                total = total * low[t, pair(i, i)]
                fit[i] = total
                res[t, 0, b, i] = total[0:8, :]
                res[t, 1, b, i] = total[8:16, :]
                explained = explained + SCALE * total * total
            ssr = jnp.maximum(total_of(8) - explained, 0.0)
            arsum[b] = arsum[b] + ssr[0:8, :] + ssr[8:16, :]
            ratio = jnp.sqrt(ssr / (gram[t, 0] + SCALE))
            sres[t, 0, b] = ratio[0:8, :]
            sres[t, 1, b] = ratio[8:16, :]
            return carried

        lax.fori_loop(0, BANDS, band, 0)

    def lanes(pz, pc):
        return pl.ds(pl.multiple_of((pz * 2 + pc) * 128, 128), 128)

    def out_copies(t, half, slot, dev):
        return (
            remote(sres.at[t, half], sstage.at[z * 2 + c], ss.at[t, half], sr.at[t, slot], dev),
            remote(res.at[t, half], coef_out.at[:, :, :, lanes(z, c)], cs.at[t, half], cr.at[t, slot], dev),
        )

    def y_results():
        slot = lax.rem(y - turn + 3, 4)
        dev = (x, pix(turn, z, c))
        return (
            remote(sres.at[0], ysres.at[slot], e_s.at[0], e_r.at[slot, 0], dev),
            remote(res.at[0], yres.at[slot], e_s.at[1], e_r.at[slot, 1], dev),
        )

    def y_arrival(slot):
        dev = (x, pix(turn, z, c))
        return (
            remote(sres.at[0], ysres.at[slot], e_s.at[0], e_r.at[slot, 0], dev),
            remote(res.at[0], yres.at[slot], e_s.at[1], e_r.at[slot, 1], dev),
        )

    def turned(i, half):
        dev = (lax.rem(y + i, 4), pix(y, row_z(0), half))
        src_score = sres.at[0, half] if i == 0 else ysres.at[i - 1, half]
        src = res.at[0, half] if i == 0 else yres.at[i - 1, half]
        return (
            remote(src_score, sstage.at[z * 2 + c], fs.at[i, half], sr.at[0, c], dev),
            remote(src, coef_out.at[:, :, :, lanes(z, c)], fc.at[i, half], cr.at[0, c], dev),
        )

    def due(s):
        ramp = s - LAG + jnp.maximum(s - RAMP, 0)
        return jnp.maximum(jnp.minimum(s - EARLY, PARTS - 1), jnp.minimum(ramp, s - 1))

    def use(n, carried):
        t = lax.div(n, PARTS)
        q = lax.rem(n, PARTS)

        @pl.when(n == 0)
        def _():
            columns()

        @pl.when(q == 0)
        def _():
            own_sums[t] = jnp.zeros((BANDS, 9, 16, 128), F32)

            @pl.when(t < CHAINED)
            def _():
                pass_sums[t] = jnp.zeros((BANDS, 9, 16, 128), F32)
                wa_copy(t).wait_recv()
                wd_copy(t).start()
                wb_copy(t).wait_recv()

            @pl.when(t >= CHAINED)
            def _():
                for tp in range(1, 4):
                    xw_copy(t, tp).wait_recv()

        @pl.when(t < CHAINED)
        def _():
            a_copy(n, t, q).wait_recv()
            moments(
                pass_sums.at[t],
                [(mid.at[fore_slot, t], midw.at[fore_slot, t], 0), (carry.at[t], carryw.at[t], back)],
                q,
            )

            @pl.when(q == PARTS - 1)
            def _():
                sum_copy(t).start()

            b_copy(n, t, q).wait_recv()

        @pl.when(t >= CHAINED)
        def _():
            for tp in range(1, 4):
                x_copy(n, t, q, tp).wait_recv()
            moments(
                own_sums.at[t],
                [(far.at[1, t], farw.at[1, t], 2), (far.at[2 - 2 * c, t], farw.at[2 - 2 * c, t], back)],
                q,
            )

        moments(
            own_sums.at[t],
            [(mid.at[home, t], midw.at[home, t], 0), (far.at[2 * c, t], farw.at[2 * c, t], fore)],
            q,
        )

        @pl.when(q == FACTOR_AT)
        def _():
            @pl.when(t < CHAINED)
            def _():
                wc_copy(t).wait_recv()
                wd_copy(t).wait_recv()

            factor(t)

        def send_results(done):
            for half in range(2):
                dev = (x, pix(y, row_z(done), half))
                for copy in out_copies(done, half, c, dev):
                    copy.start()

        @pl.when(jnp.logical_and(q == SOLVE_AT, jnp.logical_and(t > 0, t <= CHAINED)))
        def _():
            sum_copy(t - 1).wait_recv()
            solve(t - 1, True)

            @pl.when(jnp.logical_and(t == 1, turn != y))
            def _():
                for copy in y_results():
                    copy.start()

            @pl.when(t > 1)
            def _():
                send_results(t - 1)

        @pl.when(jnp.logical_and(q == PARTS - 1, t >= CHAINED))
        def _():
            solve(t, False)

            @pl.when(t < last)
            def _():
                send_results(t)

        @pl.when(jnp.logical_and(n == TURN_AT, turn == y))
        def _():
            for slot in range(3):
                for copy in y_arrival(slot):
                    copy.wait_recv()
            for i in range(4):
                for half in range(2):
                    for copy in turned(i, half):
                        copy.start()

        return carried

    def step(s, carried):
        @pl.when(jnp.logical_and(s >= PARTS, s < STEPS))
        def _():
            t = lax.div(s, PARTS)
            q = lax.rem(s, PARTS)
            y_local(s, t, q).wait()
            for tp in range(1, 4):
                y_copy(s, t, q, tp).wait_recv()

            @pl.when(t < CHAINED)
            def _():
                a_copy(s, t, q).start()
                b_copy(s, t, q).start()

            @pl.when(t >= CHAINED)
            def _():
                for tp in (2, 1, 3):
                    x_copy(s, t, q, tp).start()

            @pl.when(q == 0)
            def _():
                for tp in range(1, 4):
                    yw_copy(t, tp).wait_recv()

                @pl.when(t < CHAINED)
                def _():
                    x_codes(t)

                @pl.when(t >= CHAINED)
                def _():
                    for tp in (2, 1, 3):
                        xw_copy(t, tp).start()

            nxt = s + AHEAD

            @pl.when(nxt < STEPS)
            def _():
                @pl.when(lax.rem(nxt, PARTS) == 0)
                def _():
                    yw_start(lax.div(nxt, PARTS))

                y_start(nxt)

        lax.fori_loop(due(s - 1) + 1, due(s) + 1, use, 0)
        return carried

    lax.fori_loop(EARLY, STEPS + 1, step, 0)

    twin = (x, pix(y, z, 1 - c))
    arsrc[0] = jnp.sum(arsum[...], axis=1)

    def gather(stage, peers, first):
        copies = [
            remote(arsrc.at[stage], arbuf.at[first + n], as_.at[first + n], ar_.at[first + n], dev)
            for n, dev in enumerate(peers)
        ]
        for copy in copies:
            copy.start()
        return copies

    copies = gather(0, z_peers, 0)
    twin_copies = out_copies(last, 1 - c, 0, twin)
    for copy in twin_copies:
        copy.start()
    own = pltpu.make_async_copy(res.at[last, c], coef_out.at[:, :, :, lanes(z, c)], c_loc)
    own.start()
    sstage[z * 2 + c] = sres[last, c]
    started = list(copies)
    for copy in copies:
        copy.wait_recv()
    total = arsrc[0]
    for n in range(7):
        total = total + arbuf[n]
    arsrc[1] = total
    copies = gather(1, plane_peers, 7)
    started += copies
    for copy in copies:
        copy.wait_recv()
    total = arsrc[1]
    for n in range(15):
        total = total + arbuf[7 + n]
    total = jnp.sum(total, axis=1, keepdims=True)
    inverse = 1.0 / jnp.sqrt(total / total[7:8, :])

    for t in range(last):
        for half in range(2):
            dev = (x, pix(y, row_z(t), half))
            for copy in out_copies(t, half, half, dev):
                copy.wait_recv()
                if t > 0:
                    copy.wait_send()
    for copy in twin_copies:
        copy.wait()
    own.wait()
    for b in range(BANDS):
        factor_b = jnp.broadcast_to(inverse[b:b + 1, :], (8, 128))
        for n in range(8):
            score_out[b, :, n * 128:(n + 1) * 128] = sstage[n, b] * factor_b

    for copy in started:
        copy.wait_send()
    for tp in range(1, 4):
        d_remote(tp).wait_send()

    @pl.when(turn != y)
    def _():
        for copy in y_results():
            copy.wait_send()

    @pl.when(turn == y)
    def _():
        for i in range(4):
            for half in range(2):
                for copy in turned(i, half):
                    copy.wait_send()

    def drain(s, carried):
        t = lax.div(s, PARTS)
        q = lax.rem(s, PARTS)

        @pl.when(t > 0)
        def _():
            for tp in range(1, 4):
                y_copy(s, t, q, tp).wait_send()

        @pl.when(t < CHAINED)
        def _():
            a_copy(s, t, q).wait_send()
            b_copy(s, t, q).wait_send()

        @pl.when(t >= CHAINED)
        def _():
            for tp in range(1, 4):
                x_copy(s, t, q, tp).wait_send()

        @pl.when(q == 0)
        def _():
            @pl.when(t > 0)
            def _():
                for tp in range(1, 4):
                    yw_copy(t, tp).wait_send()

            @pl.when(t < CHAINED)
            def _():
                for copy in (wa_copy(t), wb_copy(t), wc_copy(t), wd_copy(t), sum_copy(t)):
                    copy.wait_send()

            @pl.when(t >= CHAINED)
            def _():
                for tp in range(1, 4):
                    xw_copy(t, tp).wait_send()

        return carried

    lax.fori_loop(0, STEPS, drain, 0)


def local(stack, quality, days):
    design = design_matrix(lax.optimization_barrier(jnp.broadcast_to(days[:, None], (GROUP, 128))))
    dma = pltpu.SemaphoreType.DMA
    vmem = pltpu.VMEM
    hbm = pl.BlockSpec(memory_space=pltpu.HBM)
    samples = (GROUP, BANDS, 16, 128)
    codes = (GROUP, 16, 128)
    return pl.pallas_call(
        fit_kernel,
        out_shape=(
            jax.ShapeDtypeStruct((BANDS, 8, 8, 1024), F32),
            jax.ShapeDtypeStruct((BANDS, 8, 1024), F32),
        ),
        in_specs=[hbm, hbm, hbm],
        out_specs=(hbm, pl.BlockSpec(memory_space=pltpu.VMEM)),
        scratch_shapes=[
            vmem((4, CHUNKS) + samples, BF16),
            vmem((4, CHUNKS) + codes, BF16),
            vmem((3, CHUNKS) + samples, BF16),
            vmem((3, CHUNKS) + codes, BF16),
            vmem((CHAINED,) + samples, BF16),
            vmem((CHAINED,) + codes, BF16),
            vmem((3, CHUNKS) + codes, BF16),
            vmem((GROUP, 256, 128), jnp.int32),
            vmem((4, GROUP, 128), F32),
            vmem((4, GROUP, 8, 8, 128), F32),
            vmem((CHUNKS, BANDS, 9, 16, 128), F32),
            vmem((CHAINED, BANDS, 9, 16, 128), F32),
            vmem((CHAINED, BANDS, 9, 16, 128), F32),
            vmem((CHUNKS, 36, 16, 128), F32),
            vmem((CHUNKS, 36, 16, 128), F32),
            vmem((CHUNKS, 2, BANDS, 8, 8, 128), F32),
            vmem((CHUNKS, 2, BANDS, 8, 128), F32),
            vmem((3, 2, BANDS, 8, 8, 128), F32),
            vmem((3, 2, BANDS, 8, 128), F32),
            vmem((8, BANDS, 8, 128), F32),
            vmem((8, 8, 128), F32),
            vmem((2, 8, 128), F32),
            vmem((22, 8, 128), F32),
            dma, dma((STEPS, 4)), dma,
            dma((STEPS, 3)), dma((STEPS, 3)), dma((CHUNKS, 3)), dma((CHUNKS, 3)),
            dma((STEPS,)), dma((STEPS,)), dma((STEPS,)), dma((STEPS,)), dma((STEPS, 3)), dma((STEPS, 3)),
            dma((CHUNKS,)), dma((CHUNKS,)), dma((CHUNKS, 3)), dma((CHUNKS, 3)), dma((CHUNKS,)), dma((CHUNKS,)),
            dma((3,)), dma((3,)), dma((2,)), dma((3, 2)), dma((4, 2)), dma((4, 2)),
            dma((CHUNKS, 2)), dma((CHUNKS, 2)), dma((CHUNKS, 2)), dma((CHUNKS, 2)),
            dma, dma((22,)), dma((22,)),
        ],
        compiler_params=pltpu.CompilerParams(
            collective_id=0, has_side_effects=True, vmem_limit_bytes=50 * 1024 * 1024
        ),
        name="fit",
    )(stack, quality, design)


def solution(mesh):
    return jax.shard_map(
        local,
        mesh=mesh,
        in_specs=(P("date", None, None, "pix"), P("date", None, "pix"), P("date")),
        out_specs=(P(None, None, "pix", "date"), P(None, "pix", "date")),
        check_vma=False,
    )
```

```python
import jax
import jax.numpy as jnp
from jax import lax
from jax.experimental import pallas as pl
from jax.experimental.pallas import tpu as pltpu
from jax.sharding import PartitionSpec as P

MESH = pl.DeviceIdType.MESH
F32 = jnp.float32
BF16 = jnp.bfloat16

BANDS = 7
GROUP = 16
PARTS = 4
DPART = GROUP // PARTS
CHUNKS = 4
STEPS = CHUNKS * PARTS
AHEAD = 7
RAMP = 11
EARLY = 2
LAG = 3
FACTOR_AT = 2
SOLVE_AT = 1
TURN_AT = 14
CHAINED = 3
SCALE = 12.0
PAIRS = [(i, j) for i in range(8) for j in range(i, 8)]


def pair(i, j):
    return PAIRS.index((min(i, j), max(i, j)))


def design_matrix(days):
    moment_t = days.astype(F32)
    lane = lax.broadcasted_iota(jnp.int32, (GROUP, 128), 1)
    rate = jnp.where(lane < 4, 2.0 * jnp.pi, jnp.where(lane < 6, 4.0 * jnp.pi, 6.0 * jnp.pi)).astype(F32)
    phase = rate * moment_t / 365.25
    wave = jnp.where(jnp.bitwise_and(lane, 1) == 0, jnp.cos(phase), jnp.sin(phase))
    return jnp.where(lane == 0, 1.0, jnp.where(lane == 1, (moment_t - 512.0) / 512.0, wave))


def fit_kernel(
    stack, quality, design, coef_out, score_out,
    mid, midw, far, farw, carry, carryw, wout, qv, dbuf, dfull, own_sums, pass_sums, got_sums,
    gram, low, res, sres, yres, ysres, sstage, arsum, arsrc, arbuf,
    q_sem, l_sem, d_loc, ys, yr, yws, ywr, a_s, a_r, b_s, b_r, xs, xr, wa_s, wa_r, ws, wr, sm_s, sm_r,
    ds_, dr_, e_s, e_r, fc, fs, cs, cr, ss, sr, c_loc, as_, ar_,
):
    x = lax.axis_index("date")
    p = lax.axis_index("pix")
    y = lax.div(p, 8)
    z = lax.rem(lax.div(p, 2), 4)
    c = lax.rem(p, 2)
    last = CHUNKS - 1

    def pix(py, pz, pc):
        return (py * 4 + pz) * 2 + pc

    def right(n):
        return (lax.rem(x + n, 4), p)

    fore = 1 + 2 * c
    back = 3 - 2 * c
    fore_dev = right(fore)
    back_dev = right(back)
    home = lax.rem(x - y + 4, 4)
    fore_slot = lax.rem(x + fore - y + 4, 4)
    back_slot = lax.rem(x + back - y + 4, 4)
    far_slot = lax.rem(x + 2 - y + 4, 4)
    turn = lax.rem(x + 2 * c, 4)

    y_peers = [(x, pix(lax.rem(y + t, 4), z, c)) for t in range(1, 4)]
    x_peers = [right(t) for t in range(1, 4)]
    plane_peers = [
        (lax.rem(x + n // 4, 4), pix(lax.rem(y + n % 4, 4), z, c)) for n in range(1, 16)
    ]
    z_peers = [
        (x, pix(y, lax.rem(z + e // 2, 4), lax.rem(c + e % 2, 2))) for e in range(1, 8)
    ]

    def remote(src, dst, send, recv, dev):
        return pltpu.make_async_remote_copy(
            src_ref=src, dst_ref=dst, send_sem=send, recv_sem=recv,
            device_id=dev, device_id_type=MESH,
        )

    def dates(q):
        return pl.ds(q * DPART, DPART)

    def row_z(t):
        return lax.rem(z + (1 + t) * (3 - 2 * c), 4)

    def chunk_row(ry, t):
        return pl.multiple_of(ry * 64 + row_z(t) * 16, 16)

    def first_local(q, i):
        ry = lax.rem(y + i + 2 * c, 4)
        return pltpu.make_async_copy(
            stack.at[dates(q), :, pl.ds(chunk_row(ry, 0), 16), :],
            mid.at[i, 0, dates(q)],
            l_sem.at[q, i],
        )

    def y_local(s, t, q):
        return pltpu.make_async_copy(
            stack.at[dates(q), :, pl.ds(chunk_row(y, t), 16), :],
            mid.at[0, t, dates(q)],
            l_sem.at[s, 0],
        )

    def y_copy(s, t, q, tp):
        ry = lax.rem(y + tp, 4)
        return remote(
            stack.at[dates(q), :, pl.ds(chunk_row(ry, t), 16), :],
            mid.at[4 - tp, t, dates(q)],
            ys.at[s, tp - 1], yr.at[s, 3 - tp], y_peers[tp - 1],
        )

    def yw_copy(t, tp):
        return remote(
            wout.at[tp - 1, t], midw.at[4 - tp, t],
            yws.at[t, tp - 1], ywr.at[t, 3 - tp], y_peers[tp - 1],
        )

    def a_copy(s, t, q):
        return remote(mid.at[far_slot, t, dates(q)], carry.at[t, dates(q)], a_s.at[s], a_r.at[s], fore_dev)

    def b_copy(s, t, q):
        return remote(mid.at[back_slot, t, dates(q)], far.at[2 * c, t, dates(q)], b_s.at[s], b_r.at[s], back_dev)

    def x_copy(s, t, q, tp):
        i = lax.rem(x + tp - y + 4, 4)
        return remote(
            mid.at[i, t, dates(q)], far.at[3 - tp, t, dates(q)],
            xs.at[s, tp - 1], xr.at[s, 3 - tp], x_peers[tp - 1],
        )

    def xw_copy(t, tp):
        i = lax.rem(x + tp - y + 4, 4)
        return remote(
            midw.at[i, t], farw.at[3 - tp, t],
            ws.at[t, tp - 1], wr.at[t, 3 - tp], x_peers[tp - 1],
        )

    def wa_copy(t):
        return remote(midw.at[far_slot, t], carryw.at[t], wa_s.at[t], wa_r.at[t], fore_dev)

    def wb_copy(t):
        return remote(midw.at[back_slot, t], farw.at[2 * c, t], ws.at[t, 0], wr.at[t, 2 * c], back_dev)

    def wc_copy(t):
        return remote(midw.at[fore_slot, t], farw.at[2 - 2 * c, t], ws.at[t, 1], wr.at[t, 2 - 2 * c], fore_dev)

    def wd_copy(t):
        return remote(carryw.at[t], farw.at[1, t], ws.at[t, 2], wr.at[t, 1], fore_dev)

    def sum_copy(t):
        return remote(pass_sums.at[t], got_sums.at[t], sm_s.at[t], sm_r.at[t], fore_dev)

    def d_remote(tp):
        return remote(design, dbuf.at[4 - tp], ds_.at[tp - 1], dr_.at[3 - tp], x_peers[tp - 1])

    def y_start(s):
        t = lax.div(s, PARTS)
        q = lax.rem(s, PARTS)
        for tp in (2, 1, 3):
            y_copy(s, t, q, tp).start()
        y_local(s, t, q).start()

    def yw_start(t):
        for tp in (2, 1, 3):
            yw_copy(t, tp).start()

    for i in range(4):
        first_local(0, i).start()
    q_copy = pltpu.make_async_copy(quality, qv, q_sem)
    q_copy.start()
    for q in range(1, PARTS):
        for i in range(4):
            first_local(q, i).start()
    d_copy = pltpu.make_async_copy(design, dbuf.at[0], d_loc)
    d_copy.start()

    barrier = pltpu.get_barrier_semaphore()
    for dev in y_peers + x_peers + z_peers:
        pl.semaphore_signal(barrier, inc=1, device_id=dev, device_id_type=MESH)
    pl.semaphore_wait(barrier, 13)

    def first_start(q):
        for i in range(4):
            first_local(q, i).wait()
        a_copy(q, 0, q).start()
        b_copy(q, 0, q).start()

    y_start(PARTS)
    first_start(0)
    for q in range(1, 1 + PARTS // 4):
        first_start(q)
    for tp in range(1, 4):
        d_remote(tp).start()

    def x_codes(t):
        wa_copy(t).start()
        wb_copy(t).start()
        wc_copy(t).start()

    q_copy.wait()

    def encode(n, carried):
        t = lax.div(n, 4)
        tp = lax.rem(n, 4)
        ry = lax.rem(y + tp + jnp.where(t == 0, 2 * c, 0), 4)
        bits = qv[:, pl.ds(chunk_row(ry, t), 16), :]
        level = jnp.bitwise_and(jnp.right_shift(bits, 8), 3)
        clear = jnp.bitwise_and(bits, 8) == 0
        code = jnp.where(level == 0, 12.0, jnp.where(level == 1, 6.0, jnp.where(level == 2, 4.0, 3.0)))
        code = jnp.where(clear, code, 0.0).astype(BF16)
        kept = jnp.logical_or(t == 0, tp == 0)

        @pl.when(kept)
        def _():
            midw[tp, t] = code

        @pl.when(jnp.logical_not(kept))
        def _():
            wout[tp - 1, t] = code

        return carried

    lax.fori_loop(0, 4 * CHUNKS, encode, 0)
    yw_start(1)
    x_codes(0)
    for q in range(1 + PARTS // 4, PARTS):
        first_start(q)
    for s in range(PARTS + 1, PARTS + AHEAD):
        if s % PARTS == 0:
            yw_start(s // PARTS)
        y_start(s)
    arsum[...] = jnp.zeros_like(arsum)

    def column(g, d, i):
        v = dfull[g, d, i]
        return jnp.concatenate([v, v], 0)

    def columns():
        d_copy.wait()
        for tp in range(1, 4):
            d_remote(tp).wait_recv()

        def spread(n, carried):
            g = lax.div(n, GROUP)
            d = lax.rem(n, GROUP)
            row = dbuf[g, pl.ds(d, 1), :]
            for i in range(8):
                dfull[g, d, i] = jnp.broadcast_to(row[:, i:i + 1], (8, 128))
            return carried

        lax.fori_loop(0, 4 * GROUP, spread, 0)

    def factor(t):
        codes = [midw.at[home, t]] + [farw.at[j, t] for j in range(3)]
        for rows in ((0, 1), (2, 3), (4, 5, 6, 7)):
            wanted = [(i, j) for i in rows for j in range(i, 8)]

            def add(d, sums, rows=rows, wanted=wanted):
                sums = list(sums)
                for g in range(4):
                    w = codes[g][d].astype(F32)
                    cols = {k: column(g, d, k) for k in range(rows[0], 8)}
                    for i in rows:
                        wd = w if i == 0 else w * cols[i]
                        for j in range(i, 8):
                            n = wanted.index((i, j))
                            sums[n] = sums[n] + (wd if j == 0 else wd * cols[j])
                return tuple(sums)

            sums = lax.fori_loop(
                0, GROUP, add, tuple(jnp.zeros((16, 128), F32) for _ in wanted)
            )
            for n, (i, j) in enumerate(wanted):
                gram[t, pair(i, j)] = sums[n]
        for half in (0, 8):
            lower = {}
            for j in range(8):
                total = gram[t, pair(j, j), half:half + 8, :] + SCALE
                for k in range(j):
                    total = total - lower[j, k] * lower[j, k]
                inverse = 1.0 / jnp.sqrt(total)
                low[t, pair(j, j), half:half + 8, :] = inverse
                for i in range(j + 1, 8):
                    total = gram[t, pair(j, i), half:half + 8, :]
                    for k in range(j):
                        total = total - lower[i, k] * lower[j, k]
                    lower[i, j] = total * inverse
                    low[t, pair(j, i), half:half + 8, :] = lower[i, j]
        arsum[7] = arsum[7] + gram[t, 0, 0:8, :] + gram[t, 0, 8:16, :]

    def moments(acc, refs, q):
        def band(b, carried):
            sums = [acc[b, n] for n in range(9)]
            for values, codes, g in refs:
                for dd in range(DPART):
                    d = q * DPART + dd
                    v = values[d, b].astype(F32)
                    wv = codes[d].astype(F32) * v
                    sums[8] = sums[8] + wv * v
                    sums[0] = sums[0] + wv
                    for i in range(1, 8):
                        sums[i] = sums[i] + wv * column(g, d, i)
            for n in range(9):
                acc[b, n] = sums[n]
            return carried

        lax.fori_loop(0, BANDS, band, 0)

    def solve(t, passed):
        def band(b, carried):
            def total_of(n):
                total = own_sums[t, b, n]
                return total + got_sums[t, b, n] if passed else total

            fit = []
            explained = None
            for i in range(8):
                total = total_of(i)
                for k in range(i):
                    total = total - low[t, pair(k, i)] * fit[k]
                total = total * low[t, pair(i, i)]
                fit.append(total)
                explained = total * total if i == 0 else explained + total * total
            for i in range(7, -1, -1):
                total = fit[i]
                for k in range(i + 1, 8):
                    total = total - low[t, pair(i, k)] * fit[k]
                total = total * low[t, pair(i, i)]
                fit[i] = total
                res[t, 0, b, i] = total[0:8, :]
                res[t, 1, b, i] = total[8:16, :]
                explained = explained + SCALE * total * total
            ssr = jnp.maximum(total_of(8) - explained, 0.0)
            arsum[b] = arsum[b] + ssr[0:8, :] + ssr[8:16, :]
            ratio = jnp.sqrt(ssr / (gram[t, 0] + SCALE))
            sres[t, 0, b] = ratio[0:8, :]
            sres[t, 1, b] = ratio[8:16, :]
            return carried

        lax.fori_loop(0, BANDS, band, 0)

    def lanes(pz, pc):
        return pl.ds(pl.multiple_of((pz * 2 + pc) * 128, 128), 128)

    def out_copies(t, half, slot, dev):
        return (
            remote(sres.at[t, half], sstage.at[z * 2 + c], ss.at[t, half], sr.at[t, slot], dev),
            remote(res.at[t, half], coef_out.at[:, :, :, lanes(z, c)], cs.at[t, half], cr.at[t, slot], dev),
        )

    def y_results():
        slot = lax.rem(y - turn + 3, 4)
        dev = (x, pix(turn, z, c))
        return (
            remote(sres.at[0], ysres.at[slot], e_s.at[0], e_r.at[slot, 0], dev),
            remote(res.at[0], yres.at[slot], e_s.at[1], e_r.at[slot, 1], dev),
        )

    def y_arrival(slot):
        dev = (x, pix(turn, z, c))
        return (
            remote(sres.at[0], ysres.at[slot], e_s.at[0], e_r.at[slot, 0], dev),
            remote(res.at[0], yres.at[slot], e_s.at[1], e_r.at[slot, 1], dev),
        )

    def turned(i, half):
        dev = (lax.rem(y + i, 4), pix(y, row_z(0), half))
        src_score = sres.at[0, half] if i == 0 else ysres.at[i - 1, half]
        src = res.at[0, half] if i == 0 else yres.at[i - 1, half]
        return (
            remote(src_score, sstage.at[z * 2 + c], fs.at[i, half], sr.at[0, c], dev),
            remote(src, coef_out.at[:, :, :, lanes(z, c)], fc.at[i, half], cr.at[0, c], dev),
        )

    def due(s):
        ramp = s - LAG + jnp.maximum(s - RAMP, 0)
        return jnp.maximum(jnp.minimum(s - EARLY, PARTS - 1), jnp.minimum(ramp, s - 1))

    def use(n, carried):
        t = lax.div(n, PARTS)
        q = lax.rem(n, PARTS)

        @pl.when(n == 0)
        def _():
            columns()

        @pl.when(q == 0)
        def _():
            own_sums[t] = jnp.zeros((BANDS, 9, 16, 128), F32)

            @pl.when(t < CHAINED)
            def _():
                pass_sums[t] = jnp.zeros((BANDS, 9, 16, 128), F32)
                wa_copy(t).wait_recv()
                wd_copy(t).start()
                wb_copy(t).wait_recv()

            @pl.when(t >= CHAINED)
            def _():
                for tp in range(1, 4):
                    xw_copy(t, tp).wait_recv()

        @pl.when(t < CHAINED)
        def _():
            a_copy(n, t, q).wait_recv()
            moments(
                pass_sums.at[t],
                [(mid.at[fore_slot, t], midw.at[fore_slot, t], 0), (carry.at[t], carryw.at[t], back)],
                q,
            )

            @pl.when(q == PARTS - 1)
            def _():
                sum_copy(t).start()

            b_copy(n, t, q).wait_recv()

        @pl.when(t >= CHAINED)
        def _():
            for tp in range(1, 4):
                x_copy(n, t, q, tp).wait_recv()
            moments(
                own_sums.at[t],
                [(far.at[1, t], farw.at[1, t], 2), (far.at[2 - 2 * c, t], farw.at[2 - 2 * c, t], back)],
                q,
            )

        moments(
            own_sums.at[t],
            [(mid.at[home, t], midw.at[home, t], 0), (far.at[2 * c, t], farw.at[2 * c, t], fore)],
            q,
        )

        @pl.when(q == jnp.where(t == last, 1, FACTOR_AT))
        def _():
            @pl.when(t < CHAINED)
            def _():
                wc_copy(t).wait_recv()
                wd_copy(t).wait_recv()

            factor(t)

        def send_results(done):
            for half in range(2):
                dev = (x, pix(y, row_z(done), half))
                for copy in out_copies(done, half, c, dev):
                    copy.start()

        @pl.when(jnp.logical_and(q == SOLVE_AT, jnp.logical_and(t > 0, t <= CHAINED)))
        def _():
            sum_copy(t - 1).wait_recv()
            solve(t - 1, True)

            @pl.when(jnp.logical_and(t == 1, turn != y))
            def _():
                for copy in y_results():
                    copy.start()

            @pl.when(t > 1)
            def _():
                send_results(t - 1)

        @pl.when(jnp.logical_and(q == PARTS - 1, t >= CHAINED))
        def _():
            solve(t, False)

            @pl.when(t < last)
            def _():
                send_results(t)

        @pl.when(jnp.logical_and(n == TURN_AT, turn == y))
        def _():
            for slot in range(3):
                for copy in y_arrival(slot):
                    copy.wait_recv()
            for i in range(4):
                for half in range(2):
                    for copy in turned(i, half):
                        copy.start()

        return carried

    def step(s, carried):
        @pl.when(jnp.logical_and(s >= PARTS, s < STEPS))
        def _():
            t = lax.div(s, PARTS)
            q = lax.rem(s, PARTS)
            y_local(s, t, q).wait()
            for tp in range(1, 4):
                y_copy(s, t, q, tp).wait_recv()

            @pl.when(t < CHAINED)
            def _():
                a_copy(s, t, q).start()
                b_copy(s, t, q).start()

            @pl.when(t >= CHAINED)
            def _():
                for tp in (2, 1, 3):
                    x_copy(s, t, q, tp).start()

            @pl.when(q == 0)
            def _():
                for tp in range(1, 4):
                    yw_copy(t, tp).wait_recv()

                @pl.when(t < CHAINED)
                def _():
                    x_codes(t)

                @pl.when(t >= CHAINED)
                def _():
                    for tp in (2, 1, 3):
                        xw_copy(t, tp).start()

            nxt = s + AHEAD

            @pl.when(nxt < STEPS)
            def _():
                @pl.when(lax.rem(nxt, PARTS) == 0)
                def _():
                    yw_start(lax.div(nxt, PARTS))

                y_start(nxt)

        lax.fori_loop(due(s - 1) + 1, due(s) + 1, use, 0)
        return carried

    lax.fori_loop(EARLY, STEPS + 1, step, 0)

    twin = (x, pix(y, z, 1 - c))
    arsrc[0] = jnp.sum(arsum[...], axis=1)

    def gather(stage, peers, first):
        copies = [
            remote(arsrc.at[stage], arbuf.at[first + n], as_.at[first + n], ar_.at[first + n], dev)
            for n, dev in enumerate(peers)
        ]
        for copy in copies:
            copy.start()
        return copies

    copies = gather(0, z_peers, 0)
    twin_copies = out_copies(last, 1 - c, 0, twin)
    for copy in twin_copies:
        copy.start()
    own = pltpu.make_async_copy(res.at[last, c], coef_out.at[:, :, :, lanes(z, c)], c_loc)
    own.start()
    sstage[z * 2 + c] = sres[last, c]
    started = list(copies)
    for copy in copies:
        copy.wait_recv()
    total = arsrc[0]
    for n in range(7):
        total = total + arbuf[n]
    arsrc[1] = total
    copies = gather(1, plane_peers, 7)
    started += copies
    for copy in copies:
        copy.wait_recv()
    total = arsrc[1]
    for n in range(15):
        total = total + arbuf[7 + n]
    total = jnp.sum(total, axis=1, keepdims=True)
    inverse = 1.0 / jnp.sqrt(total / total[7:8, :])

    for t in range(last):
        for half in range(2):
            dev = (x, pix(y, row_z(t), half))
            for copy in out_copies(t, half, half, dev):
                copy.wait_recv()
                if t > 0:
                    copy.wait_send()
    for copy in twin_copies:
        copy.wait()
    own.wait()
    for b in range(BANDS):
        factor_b = jnp.broadcast_to(inverse[b:b + 1, :], (8, 128))
        for n in range(8):
            score_out[b, :, n * 128:(n + 1) * 128] = sstage[n, b] * factor_b

    for copy in started:
        copy.wait_send()
    for tp in range(1, 4):
        d_remote(tp).wait_send()

    @pl.when(turn != y)
    def _():
        for copy in y_results():
            copy.wait_send()

    @pl.when(turn == y)
    def _():
        for i in range(4):
            for half in range(2):
                for copy in turned(i, half):
                    copy.wait_send()

    def drain(s, carried):
        t = lax.div(s, PARTS)
        q = lax.rem(s, PARTS)

        @pl.when(t > 0)
        def _():
            for tp in range(1, 4):
                y_copy(s, t, q, tp).wait_send()

        @pl.when(t < CHAINED)
        def _():
            a_copy(s, t, q).wait_send()
            b_copy(s, t, q).wait_send()

        @pl.when(t >= CHAINED)
        def _():
            for tp in range(1, 4):
                x_copy(s, t, q, tp).wait_send()

        @pl.when(q == 0)
        def _():
            @pl.when(t > 0)
            def _():
                for tp in range(1, 4):
                    yw_copy(t, tp).wait_send()

            @pl.when(t < CHAINED)
            def _():
                for copy in (wa_copy(t), wb_copy(t), wc_copy(t), wd_copy(t), sum_copy(t)):
                    copy.wait_send()

            @pl.when(t >= CHAINED)
            def _():
                for tp in range(1, 4):
                    xw_copy(t, tp).wait_send()

        return carried

    lax.fori_loop(0, STEPS, drain, 0)


def local(stack, quality, days):
    design = design_matrix(lax.optimization_barrier(jnp.broadcast_to(days[:, None], (GROUP, 128))))
    dma = pltpu.SemaphoreType.DMA
    vmem = pltpu.VMEM
    hbm = pl.BlockSpec(memory_space=pltpu.HBM)
    samples = (GROUP, BANDS, 16, 128)
    codes = (GROUP, 16, 128)
    return pl.pallas_call(
        fit_kernel,
        out_shape=(
            jax.ShapeDtypeStruct((BANDS, 8, 8, 1024), F32),
            jax.ShapeDtypeStruct((BANDS, 8, 1024), F32),
        ),
        in_specs=[hbm, hbm, hbm],
        out_specs=(hbm, pl.BlockSpec(memory_space=pltpu.VMEM)),
        scratch_shapes=[
            vmem((4, CHUNKS) + samples, BF16),
            vmem((4, CHUNKS) + codes, BF16),
            vmem((3, CHUNKS) + samples, BF16),
            vmem((3, CHUNKS) + codes, BF16),
            vmem((CHAINED,) + samples, BF16),
            vmem((CHAINED,) + codes, BF16),
            vmem((3, CHUNKS) + codes, BF16),
            vmem((GROUP, 256, 128), jnp.int32),
            vmem((4, GROUP, 128), F32),
            vmem((4, GROUP, 8, 8, 128), F32),
            vmem((CHUNKS, BANDS, 9, 16, 128), F32),
            vmem((CHAINED, BANDS, 9, 16, 128), F32),
            vmem((CHAINED, BANDS, 9, 16, 128), F32),
            vmem((CHUNKS, 36, 16, 128), F32),
            vmem((CHUNKS, 36, 16, 128), F32),
            vmem((CHUNKS, 2, BANDS, 8, 8, 128), F32),
            vmem((CHUNKS, 2, BANDS, 8, 128), F32),
            vmem((3, 2, BANDS, 8, 8, 128), F32),
            vmem((3, 2, BANDS, 8, 128), F32),
            vmem((8, BANDS, 8, 128), F32),
            vmem((8, 8, 128), F32),
            vmem((2, 8, 128), F32),
            vmem((22, 8, 128), F32),
            dma, dma((STEPS, 4)), dma,
            dma((STEPS, 3)), dma((STEPS, 3)), dma((CHUNKS, 3)), dma((CHUNKS, 3)),
            dma((STEPS,)), dma((STEPS,)), dma((STEPS,)), dma((STEPS,)), dma((STEPS, 3)), dma((STEPS, 3)),
            dma((CHUNKS,)), dma((CHUNKS,)), dma((CHUNKS, 3)), dma((CHUNKS, 3)), dma((CHUNKS,)), dma((CHUNKS,)),
            dma((3,)), dma((3,)), dma((2,)), dma((3, 2)), dma((4, 2)), dma((4, 2)),
            dma((CHUNKS, 2)), dma((CHUNKS, 2)), dma((CHUNKS, 2)), dma((CHUNKS, 2)),
            dma, dma((22,)), dma((22,)),
        ],
        compiler_params=pltpu.CompilerParams(
            collective_id=0, has_side_effects=True, vmem_limit_bytes=50 * 1024 * 1024
        ),
        name="fit",
    )(stack, quality, design)


def solution(mesh):
    return jax.shard_map(
        local,
        mesh=mesh,
        in_specs=(P("date", None, None, "pix"), P("date", None, "pix"), P("date")),
        out_specs=(P(None, None, "pix", "date"), P(None, "pix", "date")),
        check_vma=False,
    )
```
